256 devices in a mesh: cell: 128 (over y, x, z), gene: 2 (over core).
Axes of the slice: x: 4, y: 4, z: 8, core: 2. Of those that a mesh axis runs over, the one named last changes fastest.
Arguments:
- tiles: bfloat16 [2, 8192, 128, 128], P('gene', 'cell'), may hold values from -8 to 8
- tile_row: int32 [2, 8192], P('gene', 'cell'), may hold values from 0 to 7, as said below
- tile_col: int32 [2, 8192], P('gene', 'cell'), may hold values from 0 to 15
- tile_count: int32 [2, 128], P('gene', 'cell'), may hold values from 1 to 64, as said below
- start_basis: bfloat16 [64, 4096], P(None, 'gene'), may hold values from -0.09375 to 0.09375
Outputs:
- basis: bfloat16 [64, 131072], P(None, 'cell')
- loadings: float32 [64, 4096], P(None, ('gene', 'cell'))
The draws below stay inside these ranges and needn't reach their ends.
Inputs may be any that keep to these rules, and one draw needn't show every extreme that they name: `tile_row`: tile row of each slot, within 0 to 7; the slots of one device name distinct (row, column) pairs. `tile_count`: slots in use; for each index of gene some device uses all 64.
All inputs are finite; a program needn't handle non-finite values.
Results may differ from the reference program's by a relative error of at most 0.018.
Values may be sent and summed in bfloat16 or wider, within the bound.
A program may use at most 64 MiB of HBM per device.

```python
import jax
import jax.numpy as jnp
from jax import lax

K = 64
G = 4096
TILE = 128
ROW_BLOCKS = 8
N_CELL = 128
N_GENE = 2


strongest = 32.0


tile_scale = 0.125


def slot_places(key):
    base = jax.random.fold_in(key, 7)
    gene_blocks = G // (N_GENE * TILE)
    slot_count = ROW_BLOCKS * gene_blocks // 2
    keys = jax.random.split(base, N_GENE * N_CELL)

    def one_device(device_key):
        return jax.random.permutation(device_key, ROW_BLOCKS * gene_blocks)[:slot_count].astype(jnp.int32)
    places = jax.vmap(one_device)(keys)
    return (places.reshape(N_GENE, N_CELL * slot_count), gene_blocks)


def draw_tiles(key, part):
    places, gene_blocks = slot_places(key)
    slot_count = ROW_BLOCKS * gene_blocks // 2
    columns_all = G // TILE
    per_column = (K + columns_all - 1) // columns_all
    row_local = places // gene_blocks
    col_local = places % gene_blocks
    gene_of = jnp.arange(N_GENE, dtype=jnp.int32)[:, None]
    cell_of = (jnp.arange(N_CELL * slot_count, dtype=jnp.int32) // slot_count)[None, :]
    global_col = (gene_of * gene_blocks + col_local).reshape(N_GENE * N_CELL, slot_count).astype(jnp.int32)
    global_row = (cell_of * ROW_BLOCKS + row_local).reshape(N_GENE * N_CELL, slot_count).astype(jnp.int32)
    ladder = strongest ** (jnp.arange(K, dtype=jnp.float32) / jnp.float32(K - 1))
    order = jax.random.permutation(jax.random.fold_in(key, 21), K)
    strength = ladder[order]
    component = jnp.arange(columns_all, dtype=jnp.int32)[:, None] + columns_all * jnp.arange(per_column, dtype=jnp.int32)[None, :]
    column_strength = jnp.where(component < K, strength[jnp.minimum(component, K - 1)], 0.0)
    gene_factor = jax.random.truncated_normal(jax.random.fold_in(key, 23), -3.0, 3.0, (columns_all, per_column, TILE), jnp.float32)
    gene_factor = gene_factor / jnp.sqrt(jnp.float32(TILE))
    cell_key = jax.random.fold_in(key, 27)
    noise_key = jax.random.fold_in(key, 25)
    rise_ratio = 3.0

    def one_device(index):
        columns = global_col[index]
        rows = global_row[index]
        cell_index = (index % N_CELL).astype(jnp.float32)
        rise = jnp.float32(rise_ratio) ** (cell_index / jnp.float32(max(N_CELL - 1, 1)))
        slot_keys = jax.vmap(lambda row, col: jax.random.fold_in(cell_key, row * columns_all + col))(rows, columns)
        device_key = jax.random.fold_in(noise_key, index)
        cell_factor = jax.vmap(lambda one_key: jax.random.truncated_normal(one_key, -3.0, 3.0, (per_column, TILE), jnp.float32))(slot_keys)
        noise = jax.random.truncated_normal(device_key, -4.0, 4.0, (slot_count, TILE, TILE), jnp.float32)
        weighted = cell_factor * column_strength[columns][:, :, None]
        planted = jnp.einsum('spr,spg->srg', weighted, gene_factor[columns])
        return jnp.clip(tile_scale * rise * (noise + planted), -8.0, 8.0).astype(jnp.bfloat16)
    stacked = lax.map(one_device, jnp.arange(N_GENE * N_CELL, dtype=jnp.int32))
    return stacked.reshape(N_GENE, N_CELL * slot_count, TILE, TILE)


def draw_tile_row(key, part):
    places, gene_blocks = slot_places(key)
    return (places // gene_blocks).astype(jnp.int32)


def draw_tile_col(key, part):
    places, gene_blocks = slot_places(key)
    return (places % gene_blocks).astype(jnp.int32)


def draw_tile_count(key, part):
    slot_count = ROW_BLOCKS * (G // (N_GENE * TILE)) // 2
    first_key, second_key = jax.random.split(jax.random.fold_in(key, 11))
    lowest = max(1, slot_count // 8)
    highest = max(lowest + 1, slot_count * 7 // 8 + 1)
    counts = jax.random.randint(first_key, (N_GENE, N_CELL), lowest, highest, dtype=jnp.int32)
    fullest = jax.random.randint(second_key, (N_GENE, 1), 0, N_CELL, dtype=jnp.int32)
    return jnp.where(jnp.arange(N_CELL, dtype=jnp.int32)[None, :] == fullest, slot_count, counts).astype(jnp.int32)


def block_scale(key, shape, pieces, least, high):
    gain = 1.0
    for dim, blocks in pieces:
        steps = jax.random.uniform(jax.random.fold_in(jax.random.fold_in(key, 6), dim), (blocks,), jnp.float32, least / len(pieces), high / len(pieces))
        gain = gain * jnp.repeat(jnp.exp(steps), shape[dim] // blocks).reshape((-1,) + (1,) * (len(shape) - 1 - dim))
    return gain


def scatter_about(key, extent, width, bound, cuts=(), kind=jnp.bfloat16):
    values = jax.random.normal(key, extent, jnp.float32) * width
    if len(cuts) > 0:
        values = block_scale(key, extent, cuts, -0.22, 0.18) * values
    return jnp.clip(values, min=-bound, max=bound).astype(kind)


def setup_inputs(seed: int = 0) -> dict:
    key_list = jax.random.split(jax.random.key(seed), 6)
    tiles = draw_tiles(jax.random.fold_in(key_list[5], 71), 0)
    tile_row = draw_tile_row(jax.random.fold_in(key_list[5], 71), 0)
    tile_col = draw_tile_col(jax.random.fold_in(key_list[5], 71), 0)
    tile_count = draw_tile_count(jax.random.fold_in(key_list[5], 71), 0)
    start_basis = scatter_about(key_list[4], (K, G), G ** -0.5, 0.09375, ((1, 2),))
    return {"tiles": tiles, "tile_row": tile_row, "tile_col": tile_col, "tile_count": tile_count, "start_basis": start_basis}


def solve_lower(lower, right):
    return lax.linalg.triangular_solve(lower, right, left_side=True, lower=True)

def gram_of(scores):
    return jnp.dot(scores.astype(jnp.float32), scores.T.astype(jnp.float32), precision=lax.Precision.HIGHEST, preferred_element_type=jnp.float32)

def orthonormal(scores):
    lower_one = jnp.linalg.cholesky(gram_of(scores))
    return solve_lower(lower_one, scores)

def reference(tiles, tile_row, tile_col, tile_count, start_basis):
    slot_count = tiles.shape[1] // N_CELL
    gene_dev = G // N_GENE
    gene_blocks = gene_dev // TILE
    cell_dev = ROW_BLOCKS * TILE
    grouped = tiles.reshape(N_GENE, N_CELL, slot_count, TILE, TILE)
    rows_all = tile_row.reshape(N_GENE, N_CELL, slot_count)
    cols_all = tile_col.reshape(N_GENE, N_CELL, slot_count)

    def onehots(gene, cell):
        live_mask = (jnp.arange(slot_count) < tile_count[gene, cell]).astype(jnp.float32)
        row_hot = (rows_all[gene, cell][:, None] == jnp.arange(ROW_BLOCKS)[None, :]).astype(jnp.float32) * live_mask[:, None]
        col_hot = (cols_all[gene, cell][:, None] == jnp.arange(gene_blocks)[None, :]).astype(jnp.float32) * live_mask[:, None]
        return (row_hot, col_hot)

    def scores_of(basis):

        def one_cell(cell):
            total = jnp.zeros((K, cell_dev), jnp.float32)
            for gene in range(N_GENE):
                row_hot, col_hot = onehots(gene, cell)
                local = basis[:, gene * gene_dev:(gene + 1) * gene_dev].reshape(K, gene_blocks, TILE)
                picked = jnp.take(local, cols_all[gene, cell], axis=1).astype(jnp.float32)
                products = jnp.einsum('ksg,srg->skr', picked, grouped[gene, cell].astype(jnp.float32), precision=lax.Precision.HIGHEST)
                summed = jnp.einsum('sb,skr->kbr', row_hot, products, precision=lax.Precision.HIGHEST)
                total = total + summed.reshape(K, cell_dev)
            return total
        stacked = lax.map(one_cell, jnp.arange(N_CELL))
        return jnp.transpose(stacked, (1, 0, 2)).reshape(K, N_CELL * cell_dev)

    def loadings_of(ortho_half):
        blocks = ortho_half.reshape(K, N_CELL, cell_dev)

        def step(carry, cell):
            parts = []
            for gene in range(N_GENE):
                row_hot, col_hot = onehots(gene, cell)
                local = blocks[:, cell].reshape(K, ROW_BLOCKS, TILE)
                picked = jnp.take(local, rows_all[gene, cell], axis=1).astype(jnp.float32)
                products = jnp.einsum('ksr,srg->skg', picked, grouped[gene, cell].astype(jnp.float32), precision=lax.Precision.HIGHEST)
                summed = jnp.einsum('sb,skg->kbg', col_hot, products, precision=lax.Precision.HIGHEST)
                parts.append(summed.reshape(K, gene_dev))
            return (carry + jnp.stack(parts), None)
        start = jnp.zeros((N_GENE, K, gene_dev), jnp.float32)
        total, _ = lax.scan(step, start, jnp.arange(N_CELL))
        return jnp.transpose(total, (1, 0, 2)).reshape(K, G)
    ortho = orthonormal(scores_of(start_basis))
    middle = loadings_of(ortho.astype(jnp.bfloat16))
    ortho_two = orthonormal(scores_of(middle.astype(jnp.bfloat16)))
    loadings = loadings_of(ortho_two.astype(jnp.bfloat16))
    basis = (ortho_two * jnp.sqrt(jnp.float32(N_CELL * cell_dev))).astype(jnp.bfloat16)
    return (basis, loadings)
```

```python
import jax
import jax.numpy as jnp
from jax import lax
from jax.experimental import pallas as pl
from jax.experimental.pallas import tpu as pltpu
from jax.sharding import Mesh
from jax.sharding import PartitionSpec as P

K = 64
TILE = 128
ROW_BLOCKS = 8
COL_BLOCKS = 16
SLOTS = 64
CELLS = ROW_BLOCKS * TILE
GENES = COL_BLOCKS * TILE
NY, NX, NZ = 4, 4, 8
TOTAL_CELLS = NY * NX * NZ * CELLS
CELL = ("cell_0", "cell_1", "cell_2")
GENE_CELL = ("gene", "cell_0", "cell_1", "cell_2")
MESH = pl.DeviceIdType.MESH
F32 = jnp.float32
BF16 = jnp.bfloat16
HIGHEST = lax.Precision.HIGHEST
LANES = (((1,), (1,)), ((), ()))

PAIR, FIRST, SECOND, DEEP, GDEEP, GFIRST, GSECOND = 0, 1, 4, 7, 14, 21, 24
PER_ROUND = 27
ZGATHER, BGATHER, AGATHER = 54, 61, 64
MESSAGES = 67


def invert(gram):
    eye = (
        lax.broadcasted_iota(jnp.int32, (K, K), 0) == lax.broadcasted_iota(jnp.int32, (K, K), 1)
    ).astype(F32)
    both = jnp.concatenate([gram, eye], axis=1)
    parts = [both[8 * i : 8 * i + 8] for i in range(K // 8)]
    inner = lax.broadcasted_iota(jnp.int32, (8, 1), 0)
    scales = []
    for j in range(K):
        at, row = divmod(j, 8)
        pivot_row = parts[at][row : row + 1, :]
        pivot = pivot_row[:, j : j + 1]
        over = pivot_row * (1.0 / pivot)
        scales.append(lax.rsqrt(pivot))
        for i in range(at, K // 8):
            column = parts[i][:, j : j + 1]
            if i == at:
                column = jnp.where(inner > row, column, 0.0)
            parts[i] = parts[i] - column * over
    out = []
    for i in range(K // 8):
        scale = jnp.zeros((8, 1), F32)
        for r in range(8):
            scale = jnp.where(inner == r, scales[8 * i + r], scale)
        out.append(parts[i][:, K:] * scale)
    return jnp.concatenate(out, axis=0)


def kernel(
    inverse, tiles_any, start_ref, basis_ref, loadings_ref,
    tiles, x_ref, own, other, product, first, plane, second, deep, deep_in,
    gram, gdeep, gfirst, gsecond, gathered, mid, tile_sem, send_sem, recv_sem,
):
    y, x, z = (lax.axis_index(name) for name in CELL)
    core = lax.axis_index("gene")
    swap = 1 - core
    a = y * swap + x * core
    b = x * swap + y * core

    def on_a(d):
        at = lax.rem(a + d, 4)
        return at, (at * swap + y * core, x * swap + at * core, z, core)

    def on_b(d):
        at = lax.rem(b + d, 4)
        return at, (y * swap + at * core, at * swap + x * core, z, core)

    def on_z(d):
        at = lax.rem(z + d, NZ)
        return at, (y, x, at, core)

    partner = (y, x, z, swap)
    load = pltpu.make_async_copy(tiles_any, tiles.at[pl.ds(0, SLOTS)], tile_sem)
    load.start()

    barrier = pltpu.get_barrier_semaphore()
    peers = [partner]
    peers += [on_a(d)[1] for d in range(1, 4)] + [on_b(d)[1] for d in range(1, 4)]
    peers += [on_z(d)[1] for d in range(1, NZ)]
    for peer in peers:
        pl.semaphore_signal(barrier, inc=1, device_id=peer, device_id_type=MESH)

    tiles[SLOTS] = jnp.zeros((TILE, TILE), BF16)
    load.wait()

    def build(r, carry):
        for c in range(COL_BLOCKS):
            x_ref[pl.ds(pl.multiple_of(r * TILE, TILE), TILE), pl.ds(c * TILE, TILE)] = tiles[
                inverse[r * COL_BLOCKS + c]
            ]
        return carry

    lax.fori_loop(0, ROW_BLOCKS, build, 0)

    sent = []

    def send(src, dst, number, peer):
        copy = pltpu.make_async_remote_copy(
            src_ref=src, dst_ref=dst, send_sem=send_sem.at[number], recv_sem=recv_sem.at[number],
            device_id=peer, device_id_type=MESH,
        )
        copy.start()
        sent.append(copy)
        return copy

    def arrive(copies):
        for copy in copies:
            copy.wait_recv()

    def stored(yy, xx):
        return swap * (4 * yy + xx) + core * (4 * xx + yy)

    def round_of(r, basis):
        base = r * PER_ROUND
        own[r] = lax.dot_general(basis, x_ref[...], LANES, preferred_element_type=F32)
        if r == 0:
            pl.semaphore_wait(barrier, len(peers))
        arrive([send(own.at[r], other.at[r], base + PAIR, partner)])
        scores = own[r] + other[r]
        square = lax.dot_general(
            scores, jnp.concatenate([scores, scores], axis=0), LANES,
            precision=HIGHEST, preferred_element_type=F32,
        )
        half = lax.broadcasted_iota(jnp.int32, (K // 2, 2 * K), 1) < K
        gram[r, 0] = jnp.where(half, square[: K // 2], square[K // 2 :])
        gdeep_in = [
            send(gram.at[r, 0], gdeep.at[r, d - 1], base + GDEEP + d - 1, on_z(d)[1]) for d in range(1, NZ)
        ]
        high = scores.astype(BF16)
        low = (scores - high.astype(F32)).astype(BF16)
        doubled = jnp.dot(
            jnp.concatenate([high, low], axis=0), x_ref[...], preferred_element_type=F32
        )
        summed = doubled[:K] + doubled[K:]
        for yy in range(NY):
            for xx in range(NX):
                n = NX * yy + xx
                product[r, stored(yy, xx)] = summed[:, n * TILE : (n + 1) * TILE]
        came = []
        for d in range(1, 4):
            at, peer = on_a(d)
            came.append(send(product.at[r, pl.ds(4 * at, 4)], first.at[r, d - 1], base + FIRST + d - 1, peer))
        arrive(came)
        for j in range(4):
            plane[r, j] = product[r, 4 * a + j] + first[r, 0, j] + first[r, 1, j] + first[r, 2, j]
        came = []
        for d in range(1, 4):
            at, peer = on_b(d)
            came.append(send(plane.at[r, at], second.at[r, d - 1], base + SECOND + d - 1, peer))
        arrive(gdeep_in)
        total = gram[r, 0]
        for d in range(NZ - 1):
            total = total + gdeep[r, d]
        gram[r, 1] = total
        gcame = [send(gram.at[r, 1], gfirst.at[r, d - 1], base + GFIRST + d - 1, on_a(d)[1]) for d in range(1, 4)]
        arrive(came)
        column = plane[r, b] + second[r, 0] + second[r, 1] + second[r, 2]
        turned = jnp.transpose(jnp.concatenate([column, column], axis=0))
        lane_half = lax.broadcasted_iota(jnp.int32, (8, 2 * K), 1) < K
        for zz in range(NZ):
            deep[r, zz] = jnp.where(lane_half, turned[16 * zz : 16 * zz + 8], turned[16 * zz + 8 : 16 * zz + 16])
        came = []
        for d in range(1, NZ):
            at, peer = on_z(d)
            came.append(send(deep.at[r, at], deep_in.at[r, d - 1], base + DEEP + d - 1, peer))
        arrive(gcame)
        gram[r, 2] = gram[r, 1] + gfirst[r, 0] + gfirst[r, 1] + gfirst[r, 2]
        gcame = [send(gram.at[r, 2], gsecond.at[r, d - 1], base + GSECOND + d - 1, on_b(d)[1]) for d in range(1, 4)]
        arrive(gcame)
        packed = gram[r, 2] + gsecond[r, 0] + gsecond[r, 1] + gsecond[r, 2]
        whole = jnp.concatenate([packed[:, :K], packed[:, K:]], axis=0)
        arrive(came)
        piece = deep[r, z]
        for d in range(NZ - 1):
            piece = piece + deep_in[r, d]
        return scores, whole, piece

    def unpacked(piece):
        return jnp.concatenate([piece[:, :K], piece[:, K:]], axis=0)

    _, whole, piece = round_of(0, start_ref[...])
    gathered[z] = piece
    came = [send(gathered.at[z], gathered.at[z], ZGATHER + d - 1, on_z(d)[1]) for d in range(1, NZ)]
    lower = invert(whole)
    arrive(came)
    genes = jnp.concatenate([unpacked(gathered[zz]) for zz in range(NZ)], axis=0)
    middle = lax.dot_general(lower, genes, LANES, precision=HIGHEST, preferred_element_type=F32)
    mine = 4 * a + b
    mid[mine] = middle.astype(BF16)
    came = [send(mid.at[mine], mid.at[mine], BGATHER + d - 1, on_b(d)[1]) for d in range(1, 4)]
    arrive(came)
    rows = pl.ds(4 * a, 4)
    came = [send(mid.at[rows], mid.at[rows], AGATHER + d - 1, on_a(d)[1]) for d in range(1, 4)]
    arrive(came)
    basis = jnp.concatenate([mid[stored(n // NX, n % NX)] for n in range(NY * NX)], axis=1)

    scores, whole, piece = round_of(1, basis)
    lower = invert(whole)
    ortho = jnp.dot(lower, scores, precision=HIGHEST, preferred_element_type=F32)
    basis_ref[...] = (ortho * jnp.sqrt(F32(TOTAL_CELLS))).astype(BF16)
    loadings_ref[...] = lax.dot_general(
        lower, unpacked(piece), LANES, precision=HIGHEST, preferred_element_type=F32
    )
    for copy in sent:
        copy.wait_send()


def local(tiles, tile_row, tile_col, tile_count, start_basis):
    places = ROW_BLOCKS * COL_BLOCKS
    slot = jnp.arange(SLOTS, dtype=jnp.int32)
    place = jnp.where(slot < tile_count[0, 0], tile_row[0] * COL_BLOCKS + tile_col[0], places)
    hit = place[None, :] == jnp.arange(places, dtype=jnp.int32)[:, None]
    inverse = jnp.min(jnp.where(hit, slot[None, :], SLOTS), axis=1)
    vmem = pl.BlockSpec(memory_space=pltpu.VMEM)
    basis, loadings = pl.pallas_call(
        kernel,
        out_shape=(
            jax.ShapeDtypeStruct((K, CELLS), BF16),
            jax.ShapeDtypeStruct((K, GENES // (NY * NX * NZ)), F32),
        ),
        in_specs=[pl.BlockSpec(memory_space=pltpu.SMEM), pl.BlockSpec(memory_space=pl.ANY), vmem],
        out_specs=(vmem, vmem),
        scratch_shapes=[
            pltpu.VMEM((SLOTS + 1, TILE, TILE), BF16),
            pltpu.VMEM((CELLS, GENES), BF16),
            pltpu.VMEM((2, K, CELLS), F32),
            pltpu.VMEM((2, K, CELLS), F32),
            pltpu.VMEM((2, NY * NX, K, TILE), F32),
            pltpu.VMEM((2, 3, 4, K, TILE), F32),
            pltpu.VMEM((2, 4, K, TILE), F32),
            pltpu.VMEM((2, 3, K, TILE), F32),
            pltpu.VMEM((2, NZ, 8, TILE), F32),
            pltpu.VMEM((2, NZ - 1, 8, TILE), F32),
            pltpu.VMEM((2, 3, K // 2, 2 * K), F32),
            pltpu.VMEM((2, NZ - 1, K // 2, 2 * K), F32),
            pltpu.VMEM((2, 3, K // 2, 2 * K), F32),
            pltpu.VMEM((2, 3, K // 2, 2 * K), F32),
            pltpu.VMEM((NZ, 8, TILE), F32),
            pltpu.VMEM((NY * NX, K, TILE), BF16),
            pltpu.SemaphoreType.DMA,
            pltpu.SemaphoreType.DMA((MESSAGES,)),
            pltpu.SemaphoreType.DMA((MESSAGES,)),
        ],
        compiler_params=pltpu.CompilerParams(collective_id=0, has_side_effects=True),
    )(inverse, tiles[0], start_basis)
    return basis, loadings


def solution(mesh):
    finer = Mesh(
        mesh.devices.reshape(NY, NX, NZ, mesh.shape["gene"]), ("cell_0", "cell_1", "cell_2", "gene")
    )
    return jax.shard_map(
        local,
        mesh=finer,
        in_specs=(
            P("gene", CELL, None, None),
            P("gene", CELL),
            P("gene", CELL),
            P("gene", CELL),
            P(None, "gene"),
        ),
        out_specs=(P(None, CELL), P(None, GENE_CELL)),
        check_vma=False,
    )
```

```python
import jax
import jax.numpy as jnp
from jax import lax
from jax.experimental import pallas as pl
from jax.experimental.pallas import tpu as pltpu
from jax.sharding import Mesh
from jax.sharding import PartitionSpec as P

K = 64
TILE = 128
ROW_BLOCKS = 8
COL_BLOCKS = 16
SLOTS = 64
CELLS = ROW_BLOCKS * TILE
GENES = COL_BLOCKS * TILE
NY, NX, NZ = 4, 4, 8
PLANE = NY * NX
CHUNKS = 4
CHUNK = CELLS // CHUNKS
PAIRS = COL_BLOCKS // 2
TOTAL_CELLS = PLANE * NZ * CELLS
CELL = ("cell_0", "cell_1", "cell_2")
GENE_CELL = ("gene", "cell_0", "cell_1", "cell_2")
MESH = pl.DeviceIdType.MESH
F32 = jnp.float32
BF16 = jnp.bfloat16
LANES = (((1,), (1,)), ((), ()))

PAIR, ACROSS, DEEP, GACROSS, GDEEP = 0, 4, 20, 28, 44
PER_ROUND = 60
SPREAD = 2 * PER_ROUND
MESSAGES = SPREAD + PLANE


def hops(d):
    dy, dx = d // NX, d % NX
    return min(dy, NY - dy) + min(dx, NX - dx)


PLANE_ORDER = sorted(range(1, PLANE), key=lambda d: -hops(d))
Z_ORDER = sorted(range(1, NZ), key=lambda d: -min(d, NZ - d))


def split(value):
    high = value.astype(BF16)
    return high, (value - high.astype(F32)).astype(BF16)


def invert(packed):
    lane = lax.broadcasted_iota(jnp.int32, (8, 2 * K), 1)
    inner = lax.broadcasted_iota(jnp.int32, (8, 2 * K), 0)
    turned = pltpu.roll(packed, K, 1)
    parts = []
    for p in range(8):
        side = packed if p < 4 else turned
        at = 8 * (p % 4)
        eye = (lane == inner + (K + 8 * p)).astype(F32)
        parts.append(jnp.where(lane < K, side[at : at + 8], eye))
    out = []
    for p in range(8):
        block = parts[p]
        wide = [jnp.broadcast_to(block[:, 8 * p + j : 8 * p + j + 1], (8, 2 * K)) for j in range(8)]
        e = [[None] * 8 for _ in range(8)]
        for s in range(8):
            for j in range(s + 1):
                e[s][j] = jnp.broadcast_to(wide[j][s : s + 1, :], (8, 2 * K))
        rows = [jnp.broadcast_to(block[s : s + 1, :], (8, 2 * K)) for s in range(8)]
        lead = [
            [jnp.broadcast_to(parts[q][:, 8 * p + j : 8 * p + j + 1], (8, 2 * K)) for j in range(8)]
            for q in range(p + 1, 8)
        ]
        done = jnp.zeros((8, 2 * K), F32)
        for j in range(8):
            over = 1.0 / e[j][j]
            m = [e[s][j] * over for s in range(j + 1, 8)]
            for s in range(j + 1, 8):
                for t in range(j + 1, s + 1):
                    e[s][t] = e[s][t] - m[s - j - 1] * e[t][j]
            for s in range(j + 1, 8):
                rows[s] = rows[s] - m[s - j - 1] * rows[j]
            done = jnp.where(inner == j, rows[j] * lax.rsqrt(e[j][j]), done)
            for q in range(p + 1, 8):
                mine = lead[q - p - 1]
                for t in range(j + 1, 8):
                    mine[t] = mine[t] - mine[j] * m[t - j - 1]
                parts[q] = parts[q] - (mine[j] * over) * rows[j]
        out.append(done)
    return jnp.concatenate(out, axis=0)[:, K:]


def kernel(
    inverse_any, tiles_any, start_any, basis_ref, loadings_ref,
    inverse, tiles, x_ref, start, own, other, both, product, across, column, deep_in, pieces, pieces_in,
    gram, gacross, gdeep, lower_ref, mid, load_sem, send_sem, recv_sem,
):
    y, x, z = (lax.axis_index(name) for name in CELL)
    core = lax.axis_index("gene")
    other_core = 1 - core
    here = NX * y + x

    def in_plane(d):
        return (lax.rem(y + d // NX, NY), lax.rem(x + d % NX, NX), z, core)

    def on_z(d, which):
        return (y, x, lax.rem(z + d, NZ), which)

    partner = (y, x, z, other_core)
    loads = [
        pltpu.make_async_copy(tiles_any, tiles.at[pl.ds(0, SLOTS)], load_sem.at[0]),
        pltpu.make_async_copy(inverse_any, inverse, load_sem.at[1]),
        pltpu.make_async_copy(start_any, start, load_sem.at[2]),
    ]
    for load in loads:
        load.start()

    barrier = pltpu.get_barrier_semaphore()
    peers = [partner] + [in_plane(d) for d in range(1, PLANE)]
    peers += [on_z(d, core) for d in range(1, NZ)] + [on_z(d, other_core) for d in range(1, NZ)]
    for peer in peers:
        pl.semaphore_signal(barrier, inc=1, device_id=peer, device_id_type=MESH)

    tiles[SLOTS] = jnp.zeros((TILE, TILE), BF16)
    for load in loads:
        load.wait()
    pl.semaphore_wait(barrier, len(peers))

    def copy_of(src, dst, number, peer):
        return pltpu.make_async_remote_copy(
            src_ref=src, dst_ref=dst, send_sem=send_sem.at[number], recv_sem=recv_sem.at[number],
            device_id=peer, device_id_type=MESH,
        )

    def scores_into(r, basis_of):
        def pair_copy(i):
            return copy_of(own.at[r, i], other.at[r, i], r * PER_ROUND + PAIR + i, partner)

        def chunk(i, carry):
            at = pl.multiple_of(i * CHUNK, CHUNK)
            if r == 0:
                for k in range(2):
                    for c in range(COL_BLOCKS):
                        x_ref[pl.ds(pl.multiple_of(at + k * TILE, TILE), TILE), pl.ds(c * TILE, TILE)] = tiles[
                            inverse[(2 * i + k) * COL_BLOCKS + c]
                        ]
            own[r, i] = lax.dot_general(
                basis_of(), x_ref[pl.ds(at, CHUNK), :], LANES, preferred_element_type=F32
            )
            pair_copy(i).start()
            return carry

        lax.fori_loop(0, CHUNKS, chunk, 0)
        for i in range(CHUNKS):
            pair_copy(i).wait_recv()
            high, low = split(own[r, i] + other[r, i])
            both[:K, i * CHUNK : (i + 1) * CHUNK] = high
            both[K:, i * CHUNK : (i + 1) * CHUNK] = low

    def gram_across(r, d):
        return copy_of(gram.at[r], gacross.at[r, here], r * PER_ROUND + GACROSS + d, in_plane(d))

    def gram_deep(r, d, which):
        number = r * PER_ROUND + GDEEP + 8 * (1 - which) + d
        return copy_of(gdeep.at[r, z], gdeep.at[r, z], number, on_z(d, which))

    def gram_start(r):
        @pl.when(core == 1)
        def _():
            square = lax.dot_general(both[...], both[...], LANES, preferred_element_type=F32)
            square = square[:K] + square[K:]
            square = square + pltpu.roll(square, K, 1)
            half = lax.broadcasted_iota(jnp.int32, (K // 2, 2 * K), 1) < K
            packed = jnp.where(half, square[: K // 2], square[K // 2 :])
            gram[r] = packed
            gacross[r, here] = packed
            for d in PLANE_ORDER:
                gram_across(r, d).start()

    def gram_middle(r):
        @pl.when(core == 1)
        def _():
            for d in PLANE_ORDER:
                gram_across(r, d).wait_recv()
            total = gacross[r, 0]
            for n in range(1, PLANE):
                total = total + gacross[r, n]
            gdeep[r, z] = total
            for d in Z_ORDER:
                gram_deep(r, d, 1).start()
                gram_deep(r, d, 0).start()
            gram_deep(r, 0, 0).start()

    def gram_end(r):
        @pl.when(core == 1)
        def _():
            for d in Z_ORDER:
                gram_deep(r, d, 1).wait_recv()

        @pl.when(core == 0)
        def _():
            for d in range(NZ):
                gram_deep(r, d, 0).wait_recv()

        @pl.when(z >= 0)
        def _():
            total = gdeep[r, 0]
            for zz in range(1, NZ):
                total = total + gdeep[r, zz]
            high, low = split(invert(total))
            lower_ref[...] = jnp.concatenate([high, high, low, low], axis=1)

    def product_copy(r, n, d, peer):
        return copy_of(product.at[r, n], across.at[r, d], r * PER_ROUND + ACROSS + d, peer)

    def product_start(r):
        for dy in (2, 1, 3, 0):
            yy = lax.rem(y + dy, NY)

            def pair(i, carry):
                n = NX * yy + 2 * i
                doubled = jnp.dot(
                    both[...], x_ref[:, pl.ds(pl.multiple_of(n * TILE, 2 * TILE), 2 * TILE)],
                    preferred_element_type=F32,
                )
                summed = doubled[:K] + doubled[K:]
                for k in range(2):
                    product[r, n + k] = summed[:, k * TILE : (k + 1) * TILE]
                for k in range(2):
                    xx = 2 * i + k
                    d = NX * dy + lax.rem(xx - x + NX, NX)
                    copy = product_copy(r, n + k, d, (yy, xx, z, core))
                    if dy:
                        copy.start()
                    else:
                        pl.when(xx != x)(copy.start)
                return carry

            lax.fori_loop(0, 2, pair, 0)

    def product_middle(r):
        for d in PLANE_ORDER:
            product_copy(r, 0, d, in_plane(d)).wait_recv()
        total = product[r, here]
        for d in range(1, PLANE):
            total = total + across[r, d]
        return total

    scores_into(0, lambda: start[...])
    gram_start(0)
    product_start(0)
    gram_middle(0)
    deep_in[z] = product_middle(0)

    def whole_copy(d):
        return copy_of(deep_in.at[z], deep_in.at[z], DEEP + d, on_z(d, core))

    for d in Z_ORDER:
        whole_copy(d).start()
    gram_end(0)
    for d in Z_ORDER:
        whole_copy(d).wait_recv()
    total = deep_in[0]
    for zz in range(1, NZ):
        total = total + deep_in[zz]
    high, low = split(total)
    middle = jnp.dot(
        lower_ref[...], jnp.concatenate([high, low, high, low], axis=0), preferred_element_type=F32
    )
    mid[here] = middle.astype(BF16)

    def spread_copy(d):
        return copy_of(mid.at[here], mid.at[here], SPREAD + d, in_plane(d))

    for d in PLANE_ORDER:
        spread_copy(d).start()
    for d in PLANE_ORDER:
        spread_copy(d).wait_recv()

    scores_into(1, lambda: jnp.concatenate([mid[n] for n in range(PLANE)], axis=1))
    gram_start(1)
    product_start(1)
    gram_middle(1)
    block = product_middle(1)
    turned = jnp.transpose(jnp.concatenate([block, block], axis=0))
    lane_half = lax.broadcasted_iota(jnp.int32, (8, 2 * K), 1) < K
    for zz in range(NZ):
        pieces[zz] = jnp.where(lane_half, turned[16 * zz : 16 * zz + 8], turned[16 * zz + 8 : 16 * zz + 16])

    def piece_copy(d):
        peer = on_z(d, core)
        return copy_of(pieces.at[peer[2]], pieces_in.at[d], PER_ROUND + DEEP + d, peer)

    for d in Z_ORDER:
        piece_copy(d).start()
    gram_end(1)
    ortho = jnp.dot(
        lower_ref[...], jnp.concatenate([both[...], both[...]], axis=0), preferred_element_type=F32
    )
    basis_ref[...] = (ortho * jnp.sqrt(F32(TOTAL_CELLS))).astype(BF16)
    for d in Z_ORDER:
        piece_copy(d).wait_recv()
    piece = pieces[z]
    for d in range(1, NZ):
        piece = piece + pieces_in[d]
    high, low = split(jnp.concatenate([piece[:, :K], piece[:, K:]], axis=0))
    loadings_ref[...] = lax.dot_general(
        jnp.concatenate([high, low, high, low], axis=1), lower_ref[...], LANES, preferred_element_type=F32
    )

    for r in range(2):
        for i in range(CHUNKS):
            copy_of(own.at[r, i], other.at[r, i], r * PER_ROUND + PAIR + i, partner).wait_send()
        for d in PLANE_ORDER:
            product_copy(r, 0, d, in_plane(d)).wait_send()
    for d in Z_ORDER:
        whole_copy(d).wait_send()
        piece_copy(d).wait_send()
    for d in PLANE_ORDER:
        spread_copy(d).wait_send()

    @pl.when(core == 1)
    def _():
        for r in range(2):
            for d in PLANE_ORDER:
                gram_across(r, d).wait_send()
            for d in Z_ORDER:
                gram_deep(r, d, 1).wait_send()
            for d in range(NZ):
                gram_deep(r, d, 0).wait_send()


def local(tiles, tile_row, tile_col, tile_count, start_basis):
    places = ROW_BLOCKS * COL_BLOCKS
    slot = jnp.arange(SLOTS, dtype=jnp.int32)
    place = jnp.where(slot < tile_count[0, 0], tile_row[0] * COL_BLOCKS + tile_col[0], places)
    hit = place[None, :] == jnp.arange(places, dtype=jnp.int32)[:, None]
    inverse = jnp.min(jnp.where(hit, slot[None, :], SLOTS), axis=1)
    vmem = pl.BlockSpec(memory_space=pltpu.VMEM)
    anywhere = pl.BlockSpec(memory_space=pl.ANY)
    basis, loadings = pl.pallas_call(
        kernel,
        out_shape=(
            jax.ShapeDtypeStruct((K, CELLS), BF16),
            jax.ShapeDtypeStruct((GENES // (PLANE * NZ), K), F32),
        ),
        in_specs=[anywhere] * 3,
        out_specs=(vmem, vmem),
        scratch_shapes=[
            pltpu.SMEM((places,), jnp.int32),
            pltpu.VMEM((SLOTS + 1, TILE, TILE), BF16),
            pltpu.VMEM((CELLS, GENES), BF16),
            pltpu.VMEM((K, GENES), BF16),
            pltpu.VMEM((2, CHUNKS, K, CHUNK), F32),
            pltpu.VMEM((2, CHUNKS, K, CHUNK), F32),
            pltpu.VMEM((2 * K, CELLS), BF16),
            pltpu.VMEM((2, PLANE, K, TILE), F32),
            pltpu.VMEM((2, PLANE, K, TILE), F32),
            pltpu.VMEM((K, TILE), F32),
            pltpu.VMEM((NZ, K, TILE), F32),
            pltpu.VMEM((NZ, 8, TILE), F32),
            pltpu.VMEM((NZ, 8, TILE), F32),
            pltpu.VMEM((2, K // 2, 2 * K), F32),
            pltpu.VMEM((2, PLANE, K // 2, 2 * K), F32),
            pltpu.VMEM((2, NZ, K // 2, 2 * K), F32),
            pltpu.VMEM((K, 4 * K), BF16),
            pltpu.VMEM((PLANE, K, TILE), BF16),
            pltpu.SemaphoreType.DMA((3,)),
            pltpu.SemaphoreType.DMA((MESSAGES,)),
            pltpu.SemaphoreType.DMA((MESSAGES,)),
        ],
        compiler_params=pltpu.CompilerParams(collective_id=0, has_side_effects=True),
    )(inverse, tiles[0], start_basis)
    return basis, loadings.T


def solution(mesh):
    finer = Mesh(
        mesh.devices.reshape(NY, NX, NZ, mesh.shape["gene"]), ("cell_0", "cell_1", "cell_2", "gene")
    )
    return jax.shard_map(
        local,
        mesh=finer,
        in_specs=(
            P("gene", CELL, None, None),
            P("gene", CELL),
            P("gene", CELL),
            P("gene", CELL),
            P(None, "gene"),
        ),
        out_specs=(P(None, CELL), P(None, GENE_CELL)),
        check_vma=False,
    )
```

```python
import jax
import jax.numpy as jnp
from jax import lax
from jax.experimental import pallas as pl
from jax.experimental.pallas import tpu as pltpu
from jax.sharding import Mesh
from jax.sharding import PartitionSpec as P

K = 64
TILE = 128
ROW_BLOCKS = 8
COL_BLOCKS = 16
SLOTS = 64
CELLS = ROW_BLOCKS * TILE
GENES = COL_BLOCKS * TILE
NY, NX, NZ = 4, 4, 8
PLANE = NY * NX
CHUNKS = 2
CHUNK = CELLS // CHUNKS
PAIRS = COL_BLOCKS // 2
TOTAL_CELLS = PLANE * NZ * CELLS
CELL = ("cell_0", "cell_1", "cell_2")
GENE_CELL = ("gene", "cell_0", "cell_1", "cell_2")
MESH = pl.DeviceIdType.MESH
F32 = jnp.float32
BF16 = jnp.bfloat16
LANES = (((1,), (1,)), ((), ()))

PAIR, ACROSS, DEEP, GACROSS, GDEEP = 0, 4, 20, 28, 44
PER_ROUND = 60
SPREAD = 2 * PER_ROUND
MESSAGES = SPREAD + PLANE


def hops(d):
    dy, dx = d // NX, d % NX
    return min(dy, NY - dy) + min(dx, NX - dx)


PLANE_ORDER = sorted(range(1, PLANE), key=lambda d: -hops(d))
Z_ORDER = sorted(range(1, NZ), key=lambda d: -min(d, NZ - d))


def split(value):
    high = value.astype(BF16)
    return high, (value - high.astype(F32)).astype(BF16)


def invert(packed):
    lane = lax.broadcasted_iota(jnp.int32, (8, 2 * K), 1)
    inner = lax.broadcasted_iota(jnp.int32, (8, 2 * K), 0)
    turned = pltpu.roll(packed, K, 1)
    parts = []
    for p in range(8):
        side = packed if p < 4 else turned
        at = 8 * (p % 4)
        eye = (lane == inner + (K + 8 * p)).astype(F32)
        parts.append(jnp.where(lane < K, side[at : at + 8], eye))
    out = []
    for p in range(8):
        block = parts[p]
        wide = [jnp.broadcast_to(block[:, 8 * p + j : 8 * p + j + 1], (8, 2 * K)) for j in range(8)]
        e = [[None] * 8 for _ in range(8)]
        for s in range(8):
            for j in range(s + 1):
                e[s][j] = jnp.broadcast_to(wide[j][s : s + 1, :], (8, 2 * K))
        rows = [jnp.broadcast_to(block[s : s + 1, :], (8, 2 * K)) for s in range(8)]
        lead = [
            [jnp.broadcast_to(parts[q][:, 8 * p + j : 8 * p + j + 1], (8, 2 * K)) for j in range(8)]
            for q in range(p + 1, 8)
        ]
        done = jnp.zeros((8, 2 * K), F32)
        for j in range(8):
            over = 1.0 / e[j][j]
            m = [e[s][j] * over for s in range(j + 1, 8)]
            for s in range(j + 1, 8):
                for t in range(j + 1, s + 1):
                    e[s][t] = e[s][t] - m[s - j - 1] * e[t][j]
            for s in range(j + 1, 8):
                rows[s] = rows[s] - m[s - j - 1] * rows[j]
            done = jnp.where(inner == j, rows[j] * lax.rsqrt(e[j][j]), done)
            for q in range(p + 1, 8):
                mine = lead[q - p - 1]
                for t in range(j + 1, 8):
                    mine[t] = mine[t] - mine[j] * m[t - j - 1]
                parts[q] = parts[q] - (mine[j] * over) * rows[j]
        out.append(done)
    return jnp.concatenate(out, axis=0)[:, K:]


def finish(lower_ref, both_ref, piece_ref, basis_ref, loadings_ref):
    ortho = jnp.dot(
        lower_ref[...], jnp.concatenate([both_ref[...], both_ref[...]], axis=0), preferred_element_type=F32
    )
    basis_ref[...] = (ortho * jnp.sqrt(F32(TOTAL_CELLS))).astype(BF16)
    piece = piece_ref[...]
    high, low = split(jnp.concatenate([piece[:, :K], piece[:, K:]], axis=0))
    loadings_ref[...] = lax.dot_general(
        jnp.concatenate([high, low, high, low], axis=1), lower_ref[...], LANES, preferred_element_type=F32
    )


def kernel(
    row_any, col_any, count_any, tiles_any, start_any, lower_ref, both, piece_ref,
    places, count, inverse_v, inverse, tiles, x_ref, start, own, other, product, across, deep_in, pieces, pieces_in,
    gram, gacross, gdeep, mid, partial, load_sem, send_sem, recv_sem,
):
    y, x, z = (lax.axis_index(name) for name in CELL)
    core = lax.axis_index("gene")
    other_core = 1 - core
    here = NX * y + x

    def in_plane(d):
        return (lax.rem(y + d // NX, NY), lax.rem(x + d % NX, NX), z, core)

    def on_z(d, which):
        return (y, x, lax.rem(z + d, NZ), which)

    partner = (y, x, z, other_core)
    loads = [
        pltpu.make_async_copy(row_any, places.at[0], load_sem.at[0]),
        pltpu.make_async_copy(col_any, places.at[1], load_sem.at[1]),
        pltpu.make_async_copy(count_any, count, load_sem.at[2]),
        pltpu.make_async_copy(tiles_any, tiles.at[pl.ds(0, SLOTS)], load_sem.at[3]),
        pltpu.make_async_copy(start_any, start, load_sem.at[4]),
    ]
    for load in loads:
        load.start()

    barrier = pltpu.get_barrier_semaphore()
    peers = [partner] + [in_plane(d) for d in range(1, PLANE)]
    peers += [on_z(d, core) for d in range(1, NZ)] + [on_z(d, other_core) for d in range(1, NZ)]
    for peer in peers:
        pl.semaphore_signal(barrier, inc=1, device_id=peer, device_id_type=MESH)

    tiles[SLOTS] = jnp.zeros((TILE, TILE), BF16)
    for load in loads[:3]:
        load.wait()
    lane = lax.broadcasted_iota(jnp.int32, (1, SLOTS), 1)
    place = jnp.where(lane < count[...], places[0] * COL_BLOCKS + places[1], ROW_BLOCKS * COL_BLOCKS)
    turned = jnp.transpose(jnp.broadcast_to(jnp.concatenate([place, place], axis=1), (TILE, TILE)))[:SLOTS]
    slot = lax.broadcasted_iota(jnp.int32, (SLOTS, TILE), 0)
    spot = lax.broadcasted_iota(jnp.int32, (SLOTS, TILE), 1)
    inverse_v[...] = jnp.min(jnp.where(turned == spot, slot, SLOTS), axis=0, keepdims=True)
    lookup = pltpu.make_async_copy(inverse_v, inverse, load_sem.at[5])
    lookup.start()
    for load in loads[3:]:
        load.wait()
    lookup.wait()

    def copy_of(src, dst, number, peer):
        return pltpu.make_async_remote_copy(
            src_ref=src, dst_ref=dst, send_sem=send_sem.at[number], recv_sem=recv_sem.at[number],
            device_id=peer, device_id_type=MESH,
        )

    def pair_copy(r, i):
        return copy_of(own.at[r, i], other.at[r, i], r * PER_ROUND + PAIR + i, partner)

    def build(i):
        for k in range(CHUNK // TILE):
            row = i * CHUNK + k * TILE
            for c in range(COL_BLOCKS):
                x_ref[c, row : row + TILE] = tiles[inverse[0, row // TILE * COL_BLOCKS + c]]

    def cells_of(i, columns):
        return jnp.concatenate([x_ref[n, i * CHUNK : (i + 1) * CHUNK] for n in columns], axis=1)

    def chunk(r, i, scores_of):
        @pl.when(z >= 0)
        def _():
            if r == 0 and i == 1:
                pl.semaphore_wait(barrier, len(peers))
            if i > 0:
                pair_copy(r, i - 1).start()
            if r == 0 and i + 1 < CHUNKS:
                build(i + 1)
            own[r, i] = scores_of(i)

    def join(r):
        pair_copy(r, CHUNKS - 1).start()
        for i in range(CHUNKS):
            pair_copy(r, i).wait_recv()
            high, low = split(own[r, i] + other[r, i])
            both[:K, i * CHUNK : (i + 1) * CHUNK] = high
            both[K:, i * CHUNK : (i + 1) * CHUNK] = low

    def gram_across(r, d):
        return copy_of(gram.at[r], gacross.at[r, here], r * PER_ROUND + GACROSS + d, in_plane(d))

    def gram_deep(r, d, which):
        number = r * PER_ROUND + GDEEP + 8 * (1 - which) + d
        return copy_of(gdeep.at[r, z], gdeep.at[r, z], number, on_z(d, which))

    def gram_start(r):
        @pl.when(core == 1)
        def _():
            square = lax.dot_general(both[...], both[...], LANES, preferred_element_type=F32)
            square = square[:K] + square[K:]
            square = square + pltpu.roll(square, K, 1)
            half = lax.broadcasted_iota(jnp.int32, (K // 2, 2 * K), 1) < K
            packed = jnp.where(half, square[: K // 2], square[K // 2 :])
            gram[r] = packed
            gacross[r, here] = packed
            for d in PLANE_ORDER:
                gram_across(r, d).start()

    def gram_middle(r):
        @pl.when(core == 1)
        def _():
            for d in PLANE_ORDER:
                gram_across(r, d).wait_recv()
            total = gacross[r, 0]
            for n in range(1, PLANE):
                total = total + gacross[r, n]
            gdeep[r, z] = total
            for d in Z_ORDER:
                gram_deep(r, d, 1).start()
                gram_deep(r, d, 0).start()
            gram_deep(r, 0, 0).start()

    def gram_end(r):
        @pl.when(core == 1)
        def _():
            for d in Z_ORDER:
                gram_deep(r, d, 1).wait_recv()

        @pl.when(core == 0)
        def _():
            for d in range(NZ):
                gram_deep(r, d, 0).wait_recv()

        @pl.when(z >= 0)
        def _():
            total = gdeep[r, 0]
            for zz in range(1, NZ):
                total = total + gdeep[r, zz]
            high, low = split(invert(total))
            lower_ref[...] = jnp.concatenate([high, high, low, low], axis=1)

    def product_copy(r, n, d, peer):
        return copy_of(product.at[r, n], across.at[r, d], r * PER_ROUND + ACROSS + d, peer)

    def product_start(r):
        for dy in (2, 1, 3, 0):
            yy = lax.rem(y + dy, NY)

            @pl.when(z >= 0)
            def _():
                n = NX * yy
                doubled = jnp.dot(
                    both[...], jnp.concatenate([x_ref[n + k] for k in range(NX)], axis=1), preferred_element_type=F32
                )
                summed = doubled[:K] + doubled[K:]
                for k in range(NX):
                    product[r, n + k] = summed[:, k * TILE : (k + 1) * TILE]
                for dx in (2, 1, 3, 0):
                    if dy or dx:
                        xx = lax.rem(x + dx, NX)
                        product_copy(r, n + xx, NX * dy + dx, (yy, xx, z, core)).start()

    def product_middle(r):
        for d in PLANE_ORDER:
            product_copy(r, 0, d, in_plane(d)).wait_recv()
        total = product[r, here]
        for d in range(1, PLANE):
            total = total + across[r, d]
        return total

    build(0)
    for i in range(CHUNKS):
        chunk(
            0, i, lambda i: lax.dot_general(
                start[...], cells_of(i, range(COL_BLOCKS)), LANES, preferred_element_type=F32
            ),
        )
    join(0)
    gram_start(0)
    product_start(0)
    gram_middle(0)
    deep_in[z] = product_middle(0)

    def whole_copy(d):
        return copy_of(deep_in.at[z], deep_in.at[z], DEEP + d, on_z(d, core))

    for d in Z_ORDER:
        whole_copy(d).start()
    gram_end(0)
    for d in Z_ORDER:
        whole_copy(d).wait_recv()
    total = deep_in[0]
    for zz in range(1, NZ):
        total = total + deep_in[zz]
    high, low = split(total)
    middle = jnp.dot(
        lower_ref[...], jnp.concatenate([high, low, high, low], axis=0), preferred_element_type=F32
    )
    mid[here] = middle.astype(BF16)

    def spread_copy(d):
        return copy_of(mid.at[here], mid.at[here], SPREAD + d, in_plane(d))

    for d in PLANE_ORDER:
        spread_copy(d).start()
    def scores_with(i, offsets):
        at = [NX * lax.rem(y + NY - d // NX, NY) + lax.rem(x + NX - d % NX, NX) for d in offsets]
        return lax.dot_general(
            jnp.concatenate([mid[n] for n in at], axis=1),
            cells_of(i, at), LANES, preferred_element_type=F32,
        )

    near, far = [0] + PLANE_ORDER[:3:-1], PLANE_ORDER[:4]
    for d in near[1:]:
        spread_copy(d).wait_recv()
    for i in range(CHUNKS):
        @pl.when(z >= 0)
        def _():
            partial[i] = scores_with(i, near)

    for d in far:
        spread_copy(d).wait_recv()
    for i in range(CHUNKS):
        chunk(1, i, lambda i: partial[i] + scores_with(i, far))
    join(1)
    gram_start(1)
    product_start(1)
    gram_middle(1)
    block = product_middle(1)
    turned = jnp.transpose(jnp.concatenate([block, block], axis=0))
    lane_half = lax.broadcasted_iota(jnp.int32, (8, 2 * K), 1) < K
    for zz in range(NZ):
        pieces[zz] = jnp.where(lane_half, turned[16 * zz : 16 * zz + 8], turned[16 * zz + 8 : 16 * zz + 16])

    def piece_copy(d):
        peer = on_z(d, core)
        return copy_of(pieces.at[peer[2]], pieces_in.at[d], PER_ROUND + DEEP + d, peer)

    for d in Z_ORDER:
        piece_copy(d).start()
    gram_end(1)
    for d in Z_ORDER:
        piece_copy(d).wait_recv()
    piece = pieces[z]
    for d in range(1, NZ):
        piece = piece + pieces_in[d]
    piece_ref[...] = piece

    for r in range(2):
        for i in range(CHUNKS):
            pair_copy(r, i).wait_send()
        for d in PLANE_ORDER:
            product_copy(r, 0, d, in_plane(d)).wait_send()
    for d in Z_ORDER:
        whole_copy(d).wait_send()
        piece_copy(d).wait_send()
    for d in PLANE_ORDER:
        spread_copy(d).wait_send()

    @pl.when(core == 1)
    def _():
        for r in range(2):
            for d in PLANE_ORDER:
                gram_across(r, d).wait_send()
            for d in Z_ORDER:
                gram_deep(r, d, 1).wait_send()
            for d in range(NZ):
                gram_deep(r, d, 0).wait_send()


def local(tiles, tile_row, tile_col, tile_count, start_basis):
    vmem = pl.BlockSpec(memory_space=pltpu.VMEM)
    anywhere = pl.BlockSpec(memory_space=pltpu.HBM)
    parts = pl.pallas_call(
        kernel,
        out_shape=(
            pltpu.VMEM((K, 4 * K), BF16),
            pltpu.VMEM((2 * K, CELLS), BF16),
            pltpu.VMEM((8, TILE), F32),
        ),
        in_specs=[anywhere] * 5,
        out_specs=(vmem, vmem, vmem),
        scratch_shapes=[
            pltpu.VMEM((2, 1, SLOTS), jnp.int32),
            pltpu.VMEM((1, 1), jnp.int32),
            pltpu.VMEM((1, ROW_BLOCKS * COL_BLOCKS), jnp.int32),
            pltpu.SMEM((1, ROW_BLOCKS * COL_BLOCKS), jnp.int32),
            pltpu.VMEM((SLOTS + 1, TILE, TILE), BF16),
            pltpu.VMEM((COL_BLOCKS, CELLS, TILE), BF16),
            pltpu.VMEM((K, GENES), BF16),
            pltpu.VMEM((2, CHUNKS, K, CHUNK), F32),
            pltpu.VMEM((2, CHUNKS, K, CHUNK), F32),
            pltpu.VMEM((2, PLANE, K, TILE), F32),
            pltpu.VMEM((2, PLANE, K, TILE), F32),
            pltpu.VMEM((NZ, K, TILE), F32),
            pltpu.VMEM((NZ, 8, TILE), F32),
            pltpu.VMEM((NZ, 8, TILE), F32),
            pltpu.VMEM((2, K // 2, 2 * K), F32),
            pltpu.VMEM((2, PLANE, K // 2, 2 * K), F32),
            pltpu.VMEM((2, NZ, K // 2, 2 * K), F32),
            pltpu.VMEM((PLANE, K, TILE), BF16),
            pltpu.VMEM((CHUNKS, K, CHUNK), F32),
            pltpu.SemaphoreType.DMA((6,)),
            pltpu.SemaphoreType.DMA((MESSAGES,)),
            pltpu.SemaphoreType.DMA((MESSAGES,)),
        ],
        compiler_params=pltpu.CompilerParams(collective_id=0, has_side_effects=True),
    )(tile_row, tile_col, tile_count, tiles[0], start_basis)
    basis, loadings = pl.pallas_call(
        finish,
        out_shape=(
            jax.ShapeDtypeStruct((K, CELLS), BF16),
            jax.ShapeDtypeStruct((GENES // (PLANE * NZ), K), F32),
        ),
        in_specs=[vmem] * 3,
        out_specs=(vmem, vmem),
    )(*(pltpu.with_memory_space_constraint(part, pltpu.VMEM) for part in parts))
    return basis, loadings.T


def solution(mesh):
    finer = Mesh(
        mesh.devices.reshape(NY, NX, NZ, mesh.shape["gene"]), ("cell_0", "cell_1", "cell_2", "gene")
    )
    return jax.shard_map(
        local,
        mesh=finer,
        in_specs=(
            P("gene", CELL, None, None),
            P("gene", CELL),
            P("gene", CELL),
            P("gene", CELL),
            P(None, "gene"),
        ),
        out_specs=(P(None, CELL), P(None, GENE_CELL)),
        check_vma=False,
    )
```

```python
import jax
import jax.numpy as jnp
from jax import lax
from jax.experimental import pallas as pl
from jax.experimental.pallas import tpu as pltpu
from jax.sharding import Mesh
from jax.sharding import PartitionSpec as P

K = 64
TILE = 128
ROW_BLOCKS = 8
COL_BLOCKS = 16
SLOTS = 64
CELLS = ROW_BLOCKS * TILE
GENES = COL_BLOCKS * TILE
NY, NX, NZ = 4, 4, 8
PLANE = NY * NX
CHUNKS = 2
CHUNK = CELLS // CHUNKS
PAIRS = COL_BLOCKS // 2
TOTAL_CELLS = PLANE * NZ * CELLS
CELL = ("cell_0", "cell_1", "cell_2")
GENE_CELL = ("gene", "cell_0", "cell_1", "cell_2")
MESH = pl.DeviceIdType.MESH
F32 = jnp.float32
BF16 = jnp.bfloat16
LANES = (((1,), (1,)), ((), ()))

PAIR, ACROSS, DEEP, GACROSS, GDEEP = 0, 2, 34, 50, 66
PER_ROUND = 82
LOADS = 8
HALVES = (2, 1)
SPREAD = 2 * PER_ROUND
MESSAGES = SPREAD + PLANE


def hops(d):
    dy, dx = d // NX, d % NX
    return min(dy, NY - dy) + min(dx, NX - dx)


PLANE_ORDER = sorted(range(1, PLANE), key=lambda d: -hops(d))
Z_ORDER = sorted(range(1, NZ), key=lambda d: -min(d, NZ - d))


def split(value):
    high = value.astype(BF16)
    return high, (value - high.astype(F32)).astype(BF16)


def spread_lane(value, at):
    return jnp.take_along_axis(value, jnp.full(value.shape, at, jnp.int32), axis=1)


def invert(packed):
    lane = lax.broadcasted_iota(jnp.int32, (8, 2 * K), 1)
    inner = lax.broadcasted_iota(jnp.int32, (8, 2 * K), 0)
    turned = pltpu.roll(packed, K, 1)
    parts = []
    for p in range(8):
        side = packed if p < 4 else turned
        at = 8 * (p % 4)
        eye = (lane == inner + (K + 8 * p)).astype(F32)
        parts.append(jnp.where(lane < K, side[at : at + 8], eye))
    out = []
    for p in range(8):
        block = parts[p]
        wide = [spread_lane(block, 8 * p + j) for j in range(8)]
        e = [[None] * 8 for _ in range(8)]
        for s in range(8):
            for j in range(s + 1):
                e[s][j] = jnp.broadcast_to(wide[j][s : s + 1, :], (8, 2 * K))
        rows = [jnp.broadcast_to(block[s : s + 1, :], (8, 2 * K)) for s in range(8)]
        lead = [
            [spread_lane(parts[q], 8 * p + j) for j in range(8)]
            for q in range(p + 1, 8)
        ]
        done = jnp.zeros((8, 2 * K), F32)
        for j in range(8):
            over = 1.0 / e[j][j]
            m = [e[s][j] * over for s in range(j + 1, 8)]
            for s in range(j + 1, 8):
                for t in range(j + 1, s + 1):
                    e[s][t] = e[s][t] - m[s - j - 1] * e[t][j]
            for s in range(j + 1, 8):
                rows[s] = rows[s] - m[s - j - 1] * rows[j]
            done = jnp.where(inner == j, rows[j] * lax.rsqrt(e[j][j]), done)
            for q in range(p + 1, 8):
                mine = lead[q - p - 1]
                for t in range(j + 1, 8):
                    mine[t] = mine[t] - mine[j] * m[t - j - 1]
                parts[q] = parts[q] - (mine[j] * over) * rows[j]
        out.append(done)
    return jnp.concatenate(out, axis=0)[:, K:]


def finish(lower_ref, both_ref, piece_ref, basis_ref, loadings_ref):
    ortho = jnp.dot(
        lower_ref[...], jnp.concatenate([both_ref[...], both_ref[...]], axis=0), preferred_element_type=F32
    )
    basis_ref[...] = (ortho * jnp.sqrt(F32(TOTAL_CELLS))).astype(BF16)
    piece = piece_ref[...]
    high, low = split(jnp.concatenate([piece[:, :K], piece[:, K:]], axis=0))
    loadings_ref[...] = lax.dot_general(
        jnp.concatenate([high, low, high, low], axis=1), lower_ref[...], LANES, preferred_element_type=F32
    )


def kernel(
    row_any, col_any, count_any, tiles_any, start_any, lower_ref, both, piece_ref,
    places, count, inverse_v, inverse, tiles, x_ref, start, own, other, product, across, deep_in, pieces, pieces_in,
    gram, gacross, gdeep, mid, partial, load_sem, send_sem, recv_sem,
):
    y, x, z = (lax.axis_index(name) for name in CELL)
    core = lax.axis_index("gene")
    other_core = 1 - core
    here = NX * y + x

    def in_plane(d):
        return (lax.rem(y + d // NX, NY), lax.rem(x + d % NX, NX), z, core)

    def on_z(d, which):
        return (y, x, lax.rem(z + d, NZ), which)

    partner = (y, x, z, other_core)
    loads = [
        pltpu.make_async_copy(row_any, places.at[0], load_sem.at[0]),
        pltpu.make_async_copy(col_any, places.at[1], load_sem.at[1]),
        pltpu.make_async_copy(count_any, count, load_sem.at[2]),
        pltpu.make_async_copy(start_any, start, load_sem.at[3]),
    ]
    for n in range(LOADS):
        rows = pl.ds(n * SLOTS // LOADS, SLOTS // LOADS)
        loads.append(pltpu.make_async_copy(tiles_any.at[rows], tiles.at[rows], load_sem.at[5 + n]))
    for load in loads:
        load.start()

    barrier = pltpu.get_barrier_semaphore()
    peers = [partner] + [in_plane(d) for d in range(1, PLANE)]
    peers += [on_z(d, core) for d in range(1, NZ)] + [on_z(d, other_core) for d in range(1, NZ)]
    for peer in peers:
        pl.semaphore_signal(barrier, inc=1, device_id=peer, device_id_type=MESH)

    tiles[SLOTS] = jnp.zeros((TILE, TILE), BF16)
    for load in loads[:3]:
        load.wait()
    lane = lax.broadcasted_iota(jnp.int32, (1, SLOTS), 1)
    place = jnp.where(lane < count[...], places[0] * COL_BLOCKS + places[1], ROW_BLOCKS * COL_BLOCKS)
    turned = jnp.transpose(jnp.broadcast_to(jnp.concatenate([place, place], axis=1), (TILE, TILE)))[:SLOTS]
    slot = lax.broadcasted_iota(jnp.int32, (SLOTS, TILE), 0)
    spot = lax.broadcasted_iota(jnp.int32, (SLOTS, TILE), 1)
    inverse_v[...] = jnp.min(jnp.where(turned == spot, slot, SLOTS), axis=0, keepdims=True)
    lookup = pltpu.make_async_copy(inverse_v, inverse, load_sem.at[4])
    lookup.start()
    for load in loads[3:]:
        load.wait()
    lookup.wait()

    def copy_of(src, dst, number, peer):
        return pltpu.make_async_remote_copy(
            src_ref=src, dst_ref=dst, send_sem=send_sem.at[number], recv_sem=recv_sem.at[number],
            device_id=peer, device_id_type=MESH,
        )

    def pair_copy(r, i):
        return copy_of(own.at[r, i], other.at[r, i], r * PER_ROUND + PAIR + i, partner)

    def build(i):
        for k in range(CHUNK // TILE):
            row = i * CHUNK + k * TILE
            for c in range(COL_BLOCKS):
                x_ref[c, row : row + TILE] = tiles[inverse[0, row // TILE * COL_BLOCKS + c]]

    def cells_of(i, columns):
        return jnp.concatenate([x_ref[n, i * CHUNK : (i + 1) * CHUNK] for n in columns], axis=1)

    def chunk(r, i, scores_of):
        @pl.when(z >= 0)
        def _():
            if r == 0 and i == 1:
                pl.semaphore_wait(barrier, len(peers))
            if i > 0:
                pair_copy(r, i - 1).start()
            if r == 0 and i + 1 < CHUNKS:
                build(i + 1)
            own[r, i] = scores_of(i)

    def join(r):
        pair_copy(r, CHUNKS - 1).start()
        for i in range(CHUNKS):
            pair_copy(r, i).wait_recv()
            high, low = split(own[r, i] + other[r, i])
            both[:K, i * CHUNK : (i + 1) * CHUNK] = high
            both[K:, i * CHUNK : (i + 1) * CHUNK] = low

    def gram_across(r, d):
        return copy_of(gram.at[r], gacross.at[r, here], r * PER_ROUND + GACROSS + d, in_plane(d))

    def gram_deep(r, d, which):
        number = r * PER_ROUND + GDEEP + 8 * (1 - which) + d
        return copy_of(gdeep.at[r, z], gdeep.at[r, z], number, on_z(d, which))

    def gram_start(r):
        @pl.when(core == 1)
        def _():
            square = lax.dot_general(both[...], both[...], LANES, preferred_element_type=F32)
            square = square[:K] + square[K:]
            square = square + pltpu.roll(square, K, 1)
            half = lax.broadcasted_iota(jnp.int32, (K // 2, 2 * K), 1) < K
            packed = jnp.where(half, square[: K // 2], square[K // 2 :])
            gram[r] = packed
            gacross[r, here] = packed
            for d in PLANE_ORDER:
                gram_across(r, d).start()

    def gram_middle(r):
        @pl.when(core == 1)
        def _():
            for d in PLANE_ORDER:
                gram_across(r, d).wait_recv()
            total = gacross[r, 0]
            for n in range(1, PLANE):
                total = total + gacross[r, n]
            gdeep[r, z] = total
            for d in Z_ORDER:
                gram_deep(r, d, 1).start()
                gram_deep(r, d, 0).start()
            gram_deep(r, 0, 0).start()

    def gram_end(r):
        @pl.when(core == 1)
        def _():
            for d in Z_ORDER:
                gram_deep(r, d, 1).wait_recv()

        @pl.when(core == 0)
        def _():
            for d in range(NZ):
                gram_deep(r, d, 0).wait_recv()

        @pl.when(z >= 0)
        def _():
            total = gdeep[r, 0]
            for zz in range(1, NZ):
                total = total + gdeep[r, zz]
            high, low = split(invert(total))
            lower_ref[...] = jnp.concatenate([high, high, low, low], axis=1)

    def product_copy(r, h, n, d, peer):
        rows = pl.ds(h * K // HALVES[r], K // HALVES[r])
        number = r * PER_ROUND + ACROSS + PLANE * h + d
        return copy_of(product.at[r, n, rows], across.at[r, d, rows], number, peer)

    def product_start(r):
        def send(h, dy, dx):
            if dy or dx:
                yy, xx = lax.rem(y + dy, NY), lax.rem(x + dx, NX)
                product_copy(r, h, NX * yy + xx, NX * dy + dx, (yy, xx, z, core)).start()

        for dy in (2, 1, 3, 0):
            n = NX * lax.rem(y + dy, NY)

            @pl.when(z >= 0)
            def _():
                doubled = jnp.dot(
                    both[...], jnp.concatenate([x_ref[n + k] for k in range(NX)], axis=1), preferred_element_type=F32
                )
                summed = doubled[:K] + doubled[K:]
                for k in range(NX):
                    product[r, n + k] = summed[:, k * TILE : (k + 1) * TILE]
                for dx in (2, 1, 3, 0):
                    send(0, dy, dx)

        for h in range(1, HALVES[r]):
            for dy in (2, 1, 3, 0):
                for dx in (2, 1, 3, 0):
                    send(h, dy, dx)

    def product_middle(r, h):
        for d in PLANE_ORDER:
            product_copy(r, h, 0, d, in_plane(d)).wait_recv()
        rows = slice(h * K // HALVES[r], (h + 1) * K // HALVES[r])
        total = product[r, here, rows]
        for d in range(1, PLANE):
            total = total + across[r, d, rows]
        return total

    def left(r):
        for i in range(CHUNKS):
            pair_copy(r, i).wait_send()
        for h in range(HALVES[r]):
            for d in PLANE_ORDER:
                product_copy(r, h, 0, d, in_plane(d)).wait_send()

        @pl.when(core == 1)
        def _():
            for d in PLANE_ORDER:
                gram_across(r, d).wait_send()
            for d in Z_ORDER:
                gram_deep(r, d, 1).wait_send()
            for d in range(NZ):
                gram_deep(r, d, 0).wait_send()

    build(0)
    for i in range(CHUNKS):
        chunk(
            0, i, lambda i: lax.dot_general(
                start[...], cells_of(i, range(COL_BLOCKS)), LANES, preferred_element_type=F32
            ),
        )
    join(0)
    gram_start(0)
    product_start(0)
    gram_middle(0)
    def whole_copy(h, d):
        rows = pl.ds(h * K // HALVES[0], K // HALVES[0])
        return copy_of(deep_in.at[z, rows], deep_in.at[z, rows], DEEP + NZ * h + d, on_z(d, core))

    for h in range(HALVES[0]):
        deep_in[z, h * K // HALVES[0] : (h + 1) * K // HALVES[0]] = product_middle(0, h)
        for d in Z_ORDER:
            whole_copy(h, d).start()
    gram_end(0)
    for h in range(HALVES[0]):
        for d in Z_ORDER:
            whole_copy(h, d).wait_recv()
    total = deep_in[0]
    for zz in range(1, NZ):
        total = total + deep_in[zz]
    high, low = split(total)
    middle = jnp.dot(
        lower_ref[...], jnp.concatenate([high, low, high, low], axis=0), preferred_element_type=F32
    )
    mid[here] = middle.astype(BF16)

    def spread_copy(d):
        return copy_of(mid.at[here], mid.at[here], SPREAD + d, in_plane(d))

    for d in PLANE_ORDER:
        spread_copy(d).start()
    def scores_with(i, offsets):
        at = [NX * lax.rem(y + NY - d // NX, NY) + lax.rem(x + NX - d % NX, NX) for d in offsets]
        return lax.dot_general(
            jnp.concatenate([mid[n] for n in at], axis=1),
            cells_of(i, at), LANES, preferred_element_type=F32,
        )

    near, far = [0] + PLANE_ORDER[:3:-1], PLANE_ORDER[:4]
    for d in near[1:]:
        spread_copy(d).wait_recv()
    for i in range(CHUNKS):
        @pl.when(z >= 0)
        def _():
            partial[i] = scores_with(i, near)

    for d in far:
        spread_copy(d).wait_recv()
    for i in range(CHUNKS):
        chunk(1, i, lambda i: partial[i] + scores_with(i, far))
    join(1)
    gram_start(1)
    product_start(1)
    left(0)
    for h in range(HALVES[0]):
        for d in Z_ORDER:
            whole_copy(h, d).wait_send()
    for d in PLANE_ORDER:
        spread_copy(d).wait_send()
    gram_middle(1)
    block = product_middle(1, 0)
    turned = jnp.transpose(jnp.concatenate([block, block], axis=0))
    lane_half = lax.broadcasted_iota(jnp.int32, (8, 2 * K), 1) < K
    for zz in range(NZ):
        pieces[zz] = jnp.where(lane_half, turned[16 * zz : 16 * zz + 8], turned[16 * zz + 8 : 16 * zz + 16])

    def piece_copy(d):
        peer = on_z(d, core)
        return copy_of(pieces.at[peer[2]], pieces_in.at[d], PER_ROUND + DEEP + d, peer)

    for d in Z_ORDER:
        piece_copy(d).start()
    gram_end(1)
    for d in Z_ORDER:
        piece_copy(d).wait_recv()
    piece = pieces[z]
    for d in range(1, NZ):
        piece = piece + pieces_in[d]
    piece_ref[...] = piece

    left(1)
    for d in Z_ORDER:
        piece_copy(d).wait_send()


def local(tiles, tile_row, tile_col, tile_count, start_basis):
    vmem = pl.BlockSpec(memory_space=pltpu.VMEM)
    anywhere = pl.BlockSpec(memory_space=pltpu.HBM)
    parts = pl.pallas_call(
        kernel,
        out_shape=(
            pltpu.VMEM((K, 4 * K), BF16),
            pltpu.VMEM((2 * K, CELLS), BF16),
            pltpu.VMEM((8, TILE), F32),
        ),
        in_specs=[anywhere] * 5,
        out_specs=(vmem, vmem, vmem),
        scratch_shapes=[
            pltpu.VMEM((2, 1, SLOTS), jnp.int32),
            pltpu.VMEM((1, 1), jnp.int32),
            pltpu.VMEM((1, ROW_BLOCKS * COL_BLOCKS), jnp.int32),
            pltpu.SMEM((1, ROW_BLOCKS * COL_BLOCKS), jnp.int32),
            pltpu.VMEM((SLOTS + 1, TILE, TILE), BF16),
            pltpu.VMEM((COL_BLOCKS, CELLS, TILE), BF16),
            pltpu.VMEM((K, GENES), BF16),
            pltpu.VMEM((2, CHUNKS, K, CHUNK), F32),
            pltpu.VMEM((2, CHUNKS, K, CHUNK), F32),
            pltpu.VMEM((2, PLANE, K, TILE), F32),
            pltpu.VMEM((2, PLANE, K, TILE), F32),
            pltpu.VMEM((NZ, K, TILE), F32),
            pltpu.VMEM((NZ, 8, TILE), F32),
            pltpu.VMEM((NZ, 8, TILE), F32),
            pltpu.VMEM((2, K // 2, 2 * K), F32),
            pltpu.VMEM((2, PLANE, K // 2, 2 * K), F32),
            pltpu.VMEM((2, NZ, K // 2, 2 * K), F32),
            pltpu.VMEM((PLANE, K, TILE), BF16),
            pltpu.VMEM((CHUNKS, K, CHUNK), F32),
            pltpu.SemaphoreType.DMA((5 + LOADS,)),
            pltpu.SemaphoreType.DMA((MESSAGES,)),
            pltpu.SemaphoreType.DMA((MESSAGES,)),
        ],
        compiler_params=pltpu.CompilerParams(collective_id=0, has_side_effects=True),
    )(tile_row, tile_col, tile_count, tiles[0], start_basis)
    basis, loadings = pl.pallas_call(
        finish,
        out_shape=(
            jax.ShapeDtypeStruct((K, CELLS), BF16),
            jax.ShapeDtypeStruct((GENES // (PLANE * NZ), K), F32),
        ),
        in_specs=[vmem] * 3,
        out_specs=(vmem, vmem),
    )(*(pltpu.with_memory_space_constraint(part, pltpu.VMEM) for part in parts))
    return basis, loadings.T


def solution(mesh):
    finer = Mesh(
        mesh.devices.reshape(NY, NX, NZ, mesh.shape["gene"]), ("cell_0", "cell_1", "cell_2", "gene")
    )
    return jax.shard_map(
        local,
        mesh=finer,
        in_specs=(
            P("gene", CELL, None, None),
            P("gene", CELL),
            P("gene", CELL),
            P("gene", CELL),
            P(None, "gene"),
        ),
        out_specs=(P(None, CELL), P(None, GENE_CELL)),
        check_vma=False,
    )
```

```python
import jax
import jax.numpy as jnp
from jax import lax
from jax.experimental import pallas as pl
from jax.experimental.pallas import tpu as pltpu
from jax.sharding import Mesh
from jax.sharding import PartitionSpec as P

K = 64
TILE = 128
ROW_BLOCKS = 8
COL_BLOCKS = 16
SLOTS = 64
CELLS = ROW_BLOCKS * TILE
GENES = COL_BLOCKS * TILE
NY, NX, NZ = 4, 4, 8
PLANE = NY * NX
CHUNKS = 2
CHUNK = CELLS // CHUNKS
PAIRS = COL_BLOCKS // 2
TOTAL_CELLS = PLANE * NZ * CELLS
CELL = ("cell_0", "cell_1", "cell_2")
GENE_CELL = ("gene", "cell_0", "cell_1", "cell_2")
MESH = pl.DeviceIdType.MESH
F32 = jnp.float32
BF16 = jnp.bfloat16
LANES = (((1,), (1,)), ((), ()))

PAIR, ACROSS, DEEP, GACROSS, GDEEP = 0, 2, 34, 50, 66
PER_ROUND = 82
LOADS = 1
HALVES = (2, 1)
SPREAD = 2 * PER_ROUND
MESSAGES = SPREAD + PLANE


def hops(d):
    dy, dx = d // NX, d % NX
    return min(dy, NY - dy) + min(dx, NX - dx)


PLANE_ORDER = sorted(range(1, PLANE), key=lambda d: -hops(d))
Z_ORDER = sorted(range(1, NZ), key=lambda d: -min(d, NZ - d))


def split(value):
    high = value.astype(BF16)
    return high, (value - high.astype(F32)).astype(BF16)


def spread_lane(value, at):
    return jnp.broadcast_to(value[:, at : at + 1], value.shape)


def invert(packed):
    lane = lax.broadcasted_iota(jnp.int32, (8, 2 * K), 1)
    inner = lax.broadcasted_iota(jnp.int32, (8, 2 * K), 0)
    turned = pltpu.roll(packed, K, 1)
    parts = []
    for p in range(8):
        side = packed if p < 4 else turned
        at = 8 * (p % 4)
        eye = (lane == inner + (K + 8 * p)).astype(F32)
        parts.append(jnp.where(lane < K, side[at : at + 8], eye))
    out = []
    for p in range(8):
        block = parts[p]
        wide = [spread_lane(block, 8 * p + j) for j in range(8)]
        e = [[None] * 8 for _ in range(8)]
        for s in range(8):
            for j in range(s + 1):
                e[s][j] = jnp.broadcast_to(wide[j][s : s + 1, :], (8, 2 * K))
        rows = [jnp.broadcast_to(block[s : s + 1, :], (8, 2 * K)) for s in range(8)]
        lead = [
            [spread_lane(parts[q], 8 * p + j) for j in range(8)]
            for q in range(p + 1, 8)
        ]
        done = jnp.zeros((8, 2 * K), F32)
        for j in range(8):
            over = 1.0 / e[j][j]
            m = [e[s][j] * over for s in range(j + 1, 8)]
            for s in range(j + 1, 8):
                for t in range(j + 1, s + 1):
                    e[s][t] = e[s][t] - m[s - j - 1] * e[t][j]
            for s in range(j + 1, 8):
                rows[s] = rows[s] - m[s - j - 1] * rows[j]
            done = jnp.where(inner == j, rows[j] * lax.rsqrt(e[j][j]), done)
            for q in range(p + 1, 8):
                mine = lead[q - p - 1]
                for t in range(j + 1, 8):
                    mine[t] = mine[t] - mine[j] * m[t - j - 1]
                parts[q] = parts[q] - (mine[j] * over) * rows[j]
        out.append(done)
    return jnp.concatenate(out, axis=0)[:, K:]


def finish(lower_ref, both_ref, piece_ref, basis_ref, loadings_ref):
    ortho = jnp.dot(
        lower_ref[...], jnp.concatenate([both_ref[...], both_ref[...]], axis=0), preferred_element_type=F32
    )
    basis_ref[...] = (ortho * jnp.sqrt(F32(TOTAL_CELLS))).astype(BF16)
    piece = piece_ref[...]
    high, low = split(jnp.concatenate([piece[:, :K], piece[:, K:]], axis=0))
    loadings_ref[...] = lax.dot_general(
        jnp.concatenate([high, low, high, low], axis=1), lower_ref[...], LANES, preferred_element_type=F32
    )


def kernel(
    row_any, col_any, count_any, tiles_any, start_any, lower_ref, both, piece_ref,
    places, count, inverse_v, inverse, tiles, x_ref, start, own, other, product, across, deep_in, pieces, pieces_in,
    gram, gacross, gdeep, mid, partial, load_sem, send_sem, recv_sem,
):
    y, x, z = (lax.axis_index(name) for name in CELL)
    core = lax.axis_index("gene")
    other_core = 1 - core
    here = NX * y + x

    def in_plane(d):
        return (lax.rem(y + d // NX, NY), lax.rem(x + d % NX, NX), z, core)

    def on_z(d, which):
        return (y, x, lax.rem(z + d, NZ), which)

    partner = (y, x, z, other_core)
    loads = [
        pltpu.make_async_copy(row_any, places.at[0], load_sem.at[0]),
        pltpu.make_async_copy(col_any, places.at[1], load_sem.at[1]),
        pltpu.make_async_copy(count_any, count, load_sem.at[2]),
        pltpu.make_async_copy(start_any, start, load_sem.at[3]),
    ]
    for n in range(LOADS):
        rows = pl.ds(n * SLOTS // LOADS, SLOTS // LOADS)
        loads.append(pltpu.make_async_copy(tiles_any.at[rows], tiles.at[rows], load_sem.at[5 + n]))
    for load in loads:
        load.start()

    barrier = pltpu.get_barrier_semaphore()
    peers = [partner] + [in_plane(d) for d in range(1, PLANE)]
    peers += [on_z(d, core) for d in range(1, NZ)] + [on_z(d, other_core) for d in range(1, NZ)]
    for peer in peers:
        pl.semaphore_signal(barrier, inc=1, device_id=peer, device_id_type=MESH)

    tiles[SLOTS] = jnp.zeros((TILE, TILE), BF16)
    for load in loads[:3]:
        load.wait()
    lane = lax.broadcasted_iota(jnp.int32, (1, SLOTS), 1)
    place = jnp.where(lane < count[...], places[0] * COL_BLOCKS + places[1], ROW_BLOCKS * COL_BLOCKS)
    turned = jnp.transpose(jnp.broadcast_to(jnp.concatenate([place, place], axis=1), (TILE, TILE)))[:SLOTS]
    slot = lax.broadcasted_iota(jnp.int32, (SLOTS, TILE), 0)
    spot = lax.broadcasted_iota(jnp.int32, (SLOTS, TILE), 1)
    inverse_v[...] = jnp.min(jnp.where(turned == spot, slot, SLOTS), axis=0, keepdims=True)
    lookup = pltpu.make_async_copy(inverse_v, inverse, load_sem.at[4])
    lookup.start()
    for load in loads[3:]:
        load.wait()
    lookup.wait()

    def copy_of(src, dst, number, peer):
        return pltpu.make_async_remote_copy(
            src_ref=src, dst_ref=dst, send_sem=send_sem.at[number], recv_sem=recv_sem.at[number],
            device_id=peer, device_id_type=MESH,
        )

    def pair_copy(r, i):
        return copy_of(own.at[r, i], other.at[r, i], r * PER_ROUND + PAIR + i, partner)

    def build(i):
        for k in range(CHUNK // TILE):
            row = i * CHUNK + k * TILE
            for c in range(COL_BLOCKS):
                x_ref[c, row : row + TILE] = tiles[inverse[0, row // TILE * COL_BLOCKS + c]]

    def cells_of(i, columns):
        return jnp.concatenate([x_ref[n, i * CHUNK : (i + 1) * CHUNK] for n in columns], axis=1)

    def chunk(r, i, scores_of):
        @pl.when(z >= 0)
        def _():
            if r == 0 and i == 1:
                pl.semaphore_wait(barrier, len(peers))
            if i > 0:
                pair_copy(r, i - 1).start()
            if r == 0 and i + 1 < CHUNKS:
                build(i + 1)
            own[r, i] = scores_of(i)

    def join(r):
        pair_copy(r, CHUNKS - 1).start()
        for i in range(CHUNKS):
            pair_copy(r, i).wait_recv()
            high, low = split(own[r, i] + other[r, i])
            both[:K, i * CHUNK : (i + 1) * CHUNK] = high
            both[K:, i * CHUNK : (i + 1) * CHUNK] = low

    def gram_across(r, d):
        return copy_of(gram.at[r], gacross.at[r, here], r * PER_ROUND + GACROSS + d, in_plane(d))

    def gram_deep(r, d, which):
        number = r * PER_ROUND + GDEEP + 8 * (1 - which) + d
        return copy_of(gdeep.at[r, z], gdeep.at[r, z], number, on_z(d, which))

    def gram_start(r):
        @pl.when(core == 1)
        def _():
            square = lax.dot_general(both[...], both[...], LANES, preferred_element_type=F32)
            square = square[:K] + square[K:]
            square = square + pltpu.roll(square, K, 1)
            half = lax.broadcasted_iota(jnp.int32, (K // 2, 2 * K), 1) < K
            packed = jnp.where(half, square[: K // 2], square[K // 2 :])
            gram[r] = packed
            gacross[r, here] = packed
            for d in PLANE_ORDER:
                gram_across(r, d).start()

    def gram_middle(r):
        @pl.when(core == 1)
        def _():
            for d in PLANE_ORDER:
                gram_across(r, d).wait_recv()
            total = gacross[r, 0]
            for n in range(1, PLANE):
                total = total + gacross[r, n]
            gdeep[r, z] = total
            for d in Z_ORDER:
                gram_deep(r, d, 1).start()
                gram_deep(r, d, 0).start()
            gram_deep(r, 0, 0).start()

    def gram_end(r):
        @pl.when(core == 1)
        def _():
            for d in Z_ORDER:
                gram_deep(r, d, 1).wait_recv()

        @pl.when(core == 0)
        def _():
            for d in range(NZ):
                gram_deep(r, d, 0).wait_recv()

        @pl.when(z >= 0)
        def _():
            total = gdeep[r, 0]
            for zz in range(1, NZ):
                total = total + gdeep[r, zz]
            high, low = split(invert(total))
            lower_ref[...] = jnp.concatenate([high, high, low, low], axis=1)

    def product_copy(r, h, n, d, peer):
        rows = pl.ds(h * K // HALVES[r], K // HALVES[r])
        number = r * PER_ROUND + ACROSS + PLANE * h + d
        return copy_of(product.at[r, n, rows], across.at[r, d, rows], number, peer)

    def product_start(r):
        def send(h, dy, dx):
            if dy or dx:
                yy, xx = lax.rem(y + dy, NY), lax.rem(x + dx, NX)
                product_copy(r, h, NX * yy + xx, NX * dy + dx, (yy, xx, z, core)).start()

        for dy in (2, 1, 3, 0):
            n = NX * lax.rem(y + dy, NY)

            @pl.when(z >= 0)
            def _():
                doubled = jnp.dot(
                    both[...], jnp.concatenate([x_ref[n + k] for k in range(NX)], axis=1), preferred_element_type=F32
                )
                summed = doubled[:K] + doubled[K:]
                for k in range(NX):
                    product[r, n + k] = summed[:, k * TILE : (k + 1) * TILE]
                for dx in (2, 1, 3, 0):
                    pl.when(core >= r)(lambda dy=dy, dx=dx: send(0, dy, dx))

        @pl.when(core < r)
        def _():
            for d in PLANE_ORDER:
                send(0, d // NX, d % NX)

        for h in range(1, HALVES[r]):
            for dy in (2, 1, 3, 0):
                for dx in (2, 1, 3, 0):
                    send(h, dy, dx)

    def product_middle(r, h):
        for d in PLANE_ORDER:
            product_copy(r, h, 0, d, in_plane(d)).wait_recv()
        rows = slice(h * K // HALVES[r], (h + 1) * K // HALVES[r])
        total = product[r, here, rows]
        for d in range(1, PLANE):
            total = total + across[r, d, rows]
        return total

    def left(r):
        for i in range(CHUNKS):
            pair_copy(r, i).wait_send()
        for h in range(HALVES[r]):
            for d in PLANE_ORDER:
                product_copy(r, h, 0, d, in_plane(d)).wait_send()

        @pl.when(core == 1)
        def _():
            for d in PLANE_ORDER:
                gram_across(r, d).wait_send()
            for d in Z_ORDER:
                gram_deep(r, d, 1).wait_send()
            for d in range(NZ):
                gram_deep(r, d, 0).wait_send()

    build(0)
    for i in range(CHUNKS):
        chunk(
            0, i, lambda i: lax.dot_general(
                start[...], cells_of(i, range(COL_BLOCKS)), LANES, preferred_element_type=F32
            ),
        )
    join(0)
    gram_start(0)
    product_start(0)
    gram_middle(0)
    def whole_copy(h, d):
        rows = pl.ds(h * K // HALVES[0], K // HALVES[0])
        return copy_of(deep_in.at[z, rows], deep_in.at[z, rows], DEEP + NZ * h + d, on_z(d, core))

    for h in range(HALVES[0]):
        deep_in[z, h * K // HALVES[0] : (h + 1) * K // HALVES[0]] = product_middle(0, h)
        for d in Z_ORDER:
            whole_copy(h, d).start()
    gram_end(0)
    for h in range(HALVES[0]):
        for d in Z_ORDER:
            whole_copy(h, d).wait_recv()
    total = deep_in[0]
    for zz in range(1, NZ):
        total = total + deep_in[zz]
    high, low = split(total)
    middle = jnp.dot(
        lower_ref[...], jnp.concatenate([high, low, high, low], axis=0), preferred_element_type=F32
    )
    mid[here] = middle.astype(BF16)

    def spread_copy(d):
        return copy_of(mid.at[here], mid.at[here], SPREAD + d, in_plane(d))

    for d in PLANE_ORDER:
        spread_copy(d).start()
    def scores_with(i, offsets):
        at = [NX * lax.rem(y + NY - d // NX, NY) + lax.rem(x + NX - d % NX, NX) for d in offsets]
        return lax.dot_general(
            jnp.concatenate([mid[n] for n in at], axis=1),
            cells_of(i, at), LANES, preferred_element_type=F32,
        )

    near, far = [0] + PLANE_ORDER[:3:-1], PLANE_ORDER[:4]
    for d in near[1:]:
        spread_copy(d).wait_recv()
    for i in range(CHUNKS):
        @pl.when(z >= 0)
        def _():
            partial[i] = scores_with(i, near)

    for d in far:
        spread_copy(d).wait_recv()
    for i in range(CHUNKS):
        chunk(1, i, lambda i: partial[i] + scores_with(i, far))
    join(1)
    gram_start(1)
    product_start(1)
    gram_middle(1)
    block = product_middle(1, 0)
    turned = jnp.transpose(jnp.concatenate([block, block], axis=0))
    lane_half = lax.broadcasted_iota(jnp.int32, (8, 2 * K), 1) < K
    for zz in range(NZ):
        pieces[zz] = jnp.where(lane_half, turned[16 * zz : 16 * zz + 8], turned[16 * zz + 8 : 16 * zz + 16])

    def piece_copy(d):
        peer = on_z(d, core)
        return copy_of(pieces.at[peer[2]], pieces_in.at[d], PER_ROUND + DEEP + d, peer)

    for d in Z_ORDER:
        piece_copy(d).start()
    gram_end(1)
    for d in Z_ORDER:
        piece_copy(d).wait_recv()
    piece = pieces[z]
    for d in range(1, NZ):
        piece = piece + pieces_in[d]
    piece_ref[...] = piece

    left(0)
    for h in range(HALVES[0]):
        for d in Z_ORDER:
            whole_copy(h, d).wait_send()
    for d in PLANE_ORDER:
        spread_copy(d).wait_send()
    left(1)
    for d in Z_ORDER:
        piece_copy(d).wait_send()


def local(tiles, tile_row, tile_col, tile_count, start_basis):
    vmem = pl.BlockSpec(memory_space=pltpu.VMEM)
    anywhere = pl.BlockSpec(memory_space=pltpu.HBM)
    parts = pl.pallas_call(
        kernel,
        out_shape=(
            pltpu.VMEM((K, 4 * K), BF16),
            pltpu.VMEM((2 * K, CELLS), BF16),
            pltpu.VMEM((8, TILE), F32),
        ),
        in_specs=[anywhere] * 5,
        out_specs=(vmem, vmem, vmem),
        scratch_shapes=[
            pltpu.VMEM((2, 1, SLOTS), jnp.int32),
            pltpu.VMEM((1, 1), jnp.int32),
            pltpu.VMEM((1, ROW_BLOCKS * COL_BLOCKS), jnp.int32),
            pltpu.SMEM((1, ROW_BLOCKS * COL_BLOCKS), jnp.int32),
            pltpu.VMEM((SLOTS + 1, TILE, TILE), BF16),
            pltpu.VMEM((COL_BLOCKS, CELLS, TILE), BF16),
            pltpu.VMEM((K, GENES), BF16),
            pltpu.VMEM((2, CHUNKS, K, CHUNK), F32),
            pltpu.VMEM((2, CHUNKS, K, CHUNK), F32),
            pltpu.VMEM((2, PLANE, K, TILE), F32),
            pltpu.VMEM((2, PLANE, K, TILE), F32),
            pltpu.VMEM((NZ, K, TILE), F32),
            pltpu.VMEM((NZ, 8, TILE), F32),
            pltpu.VMEM((NZ, 8, TILE), F32),
            pltpu.VMEM((2, K // 2, 2 * K), F32),
            pltpu.VMEM((2, PLANE, K // 2, 2 * K), F32),
            pltpu.VMEM((2, NZ, K // 2, 2 * K), F32),
            pltpu.VMEM((PLANE, K, TILE), BF16),
            pltpu.VMEM((CHUNKS, K, CHUNK), F32),
            pltpu.SemaphoreType.DMA((5 + LOADS,)),
            pltpu.SemaphoreType.DMA((MESSAGES,)),
            pltpu.SemaphoreType.DMA((MESSAGES,)),
        ],
        compiler_params=pltpu.CompilerParams(collective_id=0, has_side_effects=True),
    )(tile_row, tile_col, tile_count, tiles[0], start_basis)
    basis, loadings = pl.pallas_call(
        finish,
        out_shape=(
            jax.ShapeDtypeStruct((K, CELLS), BF16),
            jax.ShapeDtypeStruct((GENES // (PLANE * NZ), K), F32),
        ),
        in_specs=[vmem] * 3,
        out_specs=(vmem, vmem),
    )(*(pltpu.with_memory_space_constraint(part, pltpu.VMEM) for part in parts))
    return basis, loadings.T


def solution(mesh):
    finer = Mesh(
        mesh.devices.reshape(NY, NX, NZ, mesh.shape["gene"]), ("cell_0", "cell_1", "cell_2", "gene")
    )
    return jax.shard_map(
        local,
        mesh=finer,
        in_specs=(
            P("gene", CELL, None, None),
            P("gene", CELL),
            P("gene", CELL),
            P("gene", CELL),
            P(None, "gene"),
        ),
        out_specs=(P(None, CELL), P(None, GENE_CELL)),
        check_vma=False,
    )
```

```python
import jax
import jax.numpy as jnp
from jax import lax
from jax.experimental import pallas as pl
from jax.experimental.pallas import tpu as pltpu
from jax.sharding import Mesh
from jax.sharding import PartitionSpec as P

K = 64
TILE = 128
ROW_BLOCKS = 8
COL_BLOCKS = 16
SLOTS = 64
CELLS = ROW_BLOCKS * TILE
GENES = COL_BLOCKS * TILE
NY, NX, NZ = 4, 4, 8
PLANE = NY * NX
CHUNKS = 2
CHUNK = CELLS // CHUNKS
PAIRS = COL_BLOCKS // 2
TOTAL_CELLS = PLANE * NZ * CELLS
CELL = ("cell_0", "cell_1", "cell_2")
GENE_CELL = ("gene", "cell_0", "cell_1", "cell_2")
MESH = pl.DeviceIdType.MESH
F32 = jnp.float32
BF16 = jnp.bfloat16
LANES = (((1,), (1,)), ((), ()))

PAIR, ACROSS, DEEP, GACROSS, GDEEP = 0, 2, 34, 50, 66
PER_ROUND = 82
LOADS = 1
HALVES = (2, 1)
SPREAD = 2 * PER_ROUND
MESSAGES = SPREAD + PLANE


def hops(d):
    dy, dx = d // NX, d % NX
    return min(dy, NY - dy) + min(dx, NX - dx)


PLANE_ORDER = sorted(range(1, PLANE), key=lambda d: -hops(d))
Z_ORDER = sorted(range(1, NZ), key=lambda d: -min(d, NZ - d))


def split(value):
    high = value.astype(BF16)
    return high, (value - high.astype(F32)).astype(BF16)


def spread_lane(value, at):
    return jnp.broadcast_to(value[:, at : at + 1], value.shape)


def pack(twice):
    quarter = lax.broadcasted_iota(jnp.int32, (8, 2 * K), 1) // 32
    ahead, back = pltpu.roll(twice, 32, 1), pltpu.roll(twice, 96, 1)

    def joined(row, sources):
        value = sources[0][row : row + 8]
        for k in range(1, 4):
            value = jnp.where(quarter == k, sources[k][row + 8 * k : row + 8 * k + 8], value)
        return value

    return jnp.concatenate(
        [joined(0, (twice, ahead) * 2), joined(32, (twice, ahead) * 2), joined(32, (back, twice) * 2)], axis=0
    )


def invert(packed):
    lane = lax.broadcasted_iota(jnp.int32, (8, 2 * K), 1)
    inner = lax.broadcasted_iota(jnp.int32, (8, 2 * K), 0)

    def moved(block, shift):
        return pltpu.roll(block, shift % 128, 1) if shift % 128 else block

    left = [moved(packed[8 * (p // 4) : 8 * (p // 4) + 8], -32 * (p % 4)) for p in range(8)]
    under = [jnp.where(lane < 32, left[4 + k], moved(packed[16:24], 32 - 32 * k)) for k in range(4)]
    turned = jnp.transpose(jnp.concatenate((left[:4] + under) * 2, axis=0))
    parts = []
    for p in range(8):
        side = jnp.where(lane < 32, left[p], turned[8 * p : 8 * p + 8]) if p < 4 else under[p - 4]
        eye = (lane == inner + (K + 8 * p)).astype(F32)
        parts.append(jnp.where(lane < K, side, eye))
    out = []
    for p in range(8):
        block = parts[p]
        wide = [spread_lane(block, 8 * p + j) for j in range(8)]
        e = [[None] * 8 for _ in range(8)]
        for s in range(8):
            for j in range(s + 1):
                e[s][j] = jnp.broadcast_to(wide[j][s : s + 1, :], (8, 2 * K))
        rows = [jnp.broadcast_to(block[s : s + 1, :], (8, 2 * K)) for s in range(8)]
        lead = [
            [spread_lane(parts[q], 8 * p + j) for j in range(8)]
            for q in range(p + 1, 8)
        ]
        done = jnp.zeros((8, 2 * K), F32)
        for j in range(8):
            over = 1.0 / e[j][j]
            m = [e[s][j] * over for s in range(j + 1, 8)]
            for s in range(j + 1, 8):
                for t in range(j + 1, s + 1):
                    e[s][t] = e[s][t] - m[s - j - 1] * e[t][j]
            for s in range(j + 1, 8):
                rows[s] = rows[s] - m[s - j - 1] * rows[j]
            done = jnp.where(inner == j, rows[j] * lax.rsqrt(e[j][j]), done)
            for q in range(p + 1, 8):
                mine = lead[q - p - 1]
                for t in range(j + 1, 8):
                    mine[t] = mine[t] - mine[j] * m[t - j - 1]
                parts[q] = parts[q] - (mine[j] * over) * rows[j]
        out.append(done)
    return jnp.concatenate(out, axis=0)[:, K:]


def finish(lower_ref, both_ref, piece_ref, basis_ref, loadings_ref):
    ortho = jnp.dot(
        lower_ref[...], jnp.concatenate([both_ref[...], both_ref[...]], axis=0), preferred_element_type=F32
    )
    basis_ref[...] = (ortho * jnp.sqrt(F32(TOTAL_CELLS))).astype(BF16)
    piece = piece_ref[...]
    high, low = split(jnp.concatenate([piece[:, :K], piece[:, K:]], axis=0))
    loadings_ref[...] = lax.dot_general(
        jnp.concatenate([high, low, high, low], axis=1), lower_ref[...], LANES, preferred_element_type=F32
    )


def kernel(
    row_any, col_any, count_any, tiles_any, start_any, lower_ref, both, piece_ref,
    places, count, inverse_v, inverse, tiles, x_ref, start, own, other, product, across, deep_in, pieces, pieces_in,
    gram, gacross, gdeep, gram_sum, mid, partial, load_sem, send_sem, recv_sem,
):
    y, x, z = (lax.axis_index(name) for name in CELL)
    core = lax.axis_index("gene")
    other_core = 1 - core
    here = NX * y + x

    def in_plane(d):
        return (lax.rem(y + d // NX, NY), lax.rem(x + d % NX, NX), z, core)

    def on_z(d, which):
        return (y, x, lax.rem(z + d, NZ), which)

    partner = (y, x, z, other_core)
    loads = [
        pltpu.make_async_copy(row_any, places.at[0], load_sem.at[0]),
        pltpu.make_async_copy(col_any, places.at[1], load_sem.at[1]),
        pltpu.make_async_copy(count_any, count, load_sem.at[2]),
        pltpu.make_async_copy(start_any, start, load_sem.at[3]),
    ]
    for n in range(LOADS):
        rows = pl.ds(n * SLOTS // LOADS, SLOTS // LOADS)
        loads.append(pltpu.make_async_copy(tiles_any.at[rows], tiles.at[rows], load_sem.at[5 + n]))
    for load in loads:
        load.start()

    barrier = pltpu.get_barrier_semaphore()
    peers = [partner] + [in_plane(d) for d in range(1, PLANE)]
    peers += [on_z(d, core) for d in range(1, NZ)] + [on_z(d, other_core) for d in range(1, NZ)]
    for peer in peers:
        pl.semaphore_signal(barrier, inc=1, device_id=peer, device_id_type=MESH)

    tiles[SLOTS] = jnp.zeros((TILE, TILE), BF16)
    for load in loads[:3]:
        load.wait()
    lane = lax.broadcasted_iota(jnp.int32, (1, SLOTS), 1)
    place = jnp.where(lane < count[...], places[0] * COL_BLOCKS + places[1], ROW_BLOCKS * COL_BLOCKS)
    turned = jnp.transpose(jnp.broadcast_to(jnp.concatenate([place, place], axis=1), (TILE, TILE)))[:SLOTS]
    slot = lax.broadcasted_iota(jnp.int32, (SLOTS, TILE), 0)
    spot = lax.broadcasted_iota(jnp.int32, (SLOTS, TILE), 1)
    inverse_v[...] = jnp.min(jnp.where(turned == spot, slot, SLOTS), axis=0, keepdims=True)
    lookup = pltpu.make_async_copy(inverse_v, inverse, load_sem.at[4])
    lookup.start()
    for load in loads[3:]:
        load.wait()
    lookup.wait()

    def copy_of(src, dst, number, peer):
        return pltpu.make_async_remote_copy(
            src_ref=src, dst_ref=dst, send_sem=send_sem.at[number], recv_sem=recv_sem.at[number],
            device_id=peer, device_id_type=MESH,
        )

    def pair_copy(r, i):
        return copy_of(own.at[r, i], other.at[r, i], r * PER_ROUND + PAIR + i, partner)

    def build(i):
        for k in range(CHUNK // TILE):
            row = i * CHUNK + k * TILE
            for c in range(COL_BLOCKS):
                x_ref[c, row : row + TILE] = tiles[inverse[0, row // TILE * COL_BLOCKS + c]]

    def cells_of(i, columns):
        return jnp.concatenate([x_ref[n, i * CHUNK : (i + 1) * CHUNK] for n in columns], axis=1)

    def chunk(r, i, scores_of):
        @pl.when(z >= 0)
        def _():
            if r == 0 and i == 1:
                pl.semaphore_wait(barrier, len(peers))
            if i > 0:
                pair_copy(r, i - 1).start()
            if r == 0 and i + 1 < CHUNKS:
                build(i + 1)
            own[r, i] = scores_of(i)

    def join(r):
        pair_copy(r, CHUNKS - 1).start()
        for i in range(CHUNKS):
            pair_copy(r, i).wait_recv()
            high, low = split(own[r, i] + other[r, i])
            both[:K, i * CHUNK : (i + 1) * CHUNK] = high
            both[K:, i * CHUNK : (i + 1) * CHUNK] = low

    def gram_across(r, d):
        return copy_of(gram.at[r], gacross.at[r, here], r * PER_ROUND + GACROSS + d, in_plane(d))

    def gram_deep(r, d, which):
        number = r * PER_ROUND + GDEEP + 8 * (1 - which) + d
        return copy_of(gdeep.at[r, z], gdeep.at[r, z], number, on_z(d, which))

    def gram_start(r):
        @pl.when(core == 1)
        def _():
            square = lax.dot_general(both[...], both[...], LANES, preferred_element_type=F32)
            square = square[:K] + square[K:]
            square = square + pltpu.roll(square, K, 1)
            packed = pack(square)
            gram[r] = packed
            gacross[r, here] = packed
            for d in PLANE_ORDER:
                gram_across(r, d).start()

    def gram_middle(r):
        @pl.when(core == 1)
        def _():
            for d in PLANE_ORDER:
                gram_across(r, d).wait_recv()
            total = gacross[r, 0]
            for n in range(1, PLANE):
                total = total + gacross[r, n]
            gdeep[r, z] = total
            for d in Z_ORDER:
                gram_deep(r, d, 1).start()
                if r == 1:
                    gram_deep(r, d, 0).start()
            if r == 1:
                gram_deep(r, 0, 0).start()

    def gram_pair():
        return copy_of(gram_sum, gram_sum, GDEEP + NZ, partner)

    def gram_end(r):
        @pl.when(core == 1)
        def _():
            for d in Z_ORDER:
                gram_deep(r, d, 1).wait_recv()
            if r == 0:
                total = gdeep[r, 0]
                for zz in range(1, NZ):
                    total = total + gdeep[r, zz]
                gram_sum[...] = total
                gram_pair().start()

        @pl.when(core == 0)
        def _():
            if r == 0:
                gram_pair().wait_recv()
            else:
                for d in range(NZ):
                    gram_deep(r, d, 0).wait_recv()

        @pl.when(z >= 0)
        def _():
            if r == 0:
                total = gram_sum[...]
            else:
                total = gdeep[r, 0]
                for zz in range(1, NZ):
                    total = total + gdeep[r, zz]
            high, low = split(invert(total))
            lower_ref[...] = jnp.concatenate([high, high, low, low], axis=1)

    def product_copy(r, h, n, d, peer):
        rows = pl.ds(h * K // HALVES[r], K // HALVES[r])
        number = r * PER_ROUND + ACROSS + PLANE * h + d
        return copy_of(product.at[r, n, rows], across.at[r, d, rows], number, peer)

    def product_start(r):
        def send(h, dy, dx):
            if dy or dx:
                yy, xx = lax.rem(y + dy, NY), lax.rem(x + dx, NX)
                product_copy(r, h, NX * yy + xx, NX * dy + dx, (yy, xx, z, core)).start()

        for dy in (2, 1, 3, 0):
            n = NX * lax.rem(y + dy, NY)

            @pl.when(z >= 0)
            def _():
                doubled = jnp.dot(
                    both[...], jnp.concatenate([x_ref[n + k] for k in range(NX)], axis=1), preferred_element_type=F32
                )
                summed = doubled[:K] + doubled[K:]
                for k in range(NX):
                    product[r, n + k] = summed[:, k * TILE : (k + 1) * TILE]
                for dx in (2, 1, 3, 0):
                    pl.when(core >= r)(lambda dy=dy, dx=dx: send(0, dy, dx))

        @pl.when(core < r)
        def _():
            for d in PLANE_ORDER:
                send(0, d // NX, d % NX)

        for h in range(1, HALVES[r]):
            for d in PLANE_ORDER:
                send(h, d // NX, d % NX)

    def product_middle(r, h):
        for d in PLANE_ORDER:
            product_copy(r, h, 0, d, in_plane(d)).wait_recv()
        rows = slice(h * K // HALVES[r], (h + 1) * K // HALVES[r])
        total = product[r, here, rows]
        for d in range(1, PLANE):
            total = total + across[r, d, rows]
        return total

    def left(r):
        for i in range(CHUNKS):
            pair_copy(r, i).wait_send()
        for h in range(HALVES[r]):
            for d in PLANE_ORDER:
                product_copy(r, h, 0, d, in_plane(d)).wait_send()

        @pl.when(core == 1)
        def _():
            for d in PLANE_ORDER:
                gram_across(r, d).wait_send()
            for d in Z_ORDER:
                gram_deep(r, d, 1).wait_send()
            if r == 0:
                gram_pair().wait_send()
            else:
                for d in range(NZ):
                    gram_deep(r, d, 0).wait_send()

    build(0)
    for i in range(CHUNKS):
        chunk(
            0, i, lambda i: lax.dot_general(
                start[...], cells_of(i, range(COL_BLOCKS)), LANES, preferred_element_type=F32
            ),
        )
    join(0)
    gram_start(0)
    product_start(0)
    gram_middle(0)
    def whole_copy(h, d):
        rows = pl.ds(h * K // HALVES[0], K // HALVES[0])
        return copy_of(deep_in.at[z, rows], deep_in.at[z, rows], DEEP + NZ * h + d, on_z(d, core))

    for h in range(HALVES[0]):
        deep_in[z, h * K // HALVES[0] : (h + 1) * K // HALVES[0]] = product_middle(0, h)
        for d in Z_ORDER:
            whole_copy(h, d).start()
    gram_end(0)
    for h in range(HALVES[0]):
        for d in Z_ORDER:
            whole_copy(h, d).wait_recv()
    total = deep_in[0]
    for zz in range(1, NZ):
        total = total + deep_in[zz]
    high, low = split(total)
    middle = jnp.dot(
        lower_ref[...], jnp.concatenate([high, low, high, low], axis=0), preferred_element_type=F32
    )
    mid[here] = middle.astype(BF16)

    def spread_copy(d):
        return copy_of(mid.at[here], mid.at[here], SPREAD + d, in_plane(d))

    for d in PLANE_ORDER:
        spread_copy(d).start()
    def scores_with(i, offsets):
        at = [NX * lax.rem(y + NY - d // NX, NY) + lax.rem(x + NX - d % NX, NX) for d in offsets]
        return lax.dot_general(
            jnp.concatenate([mid[n] for n in at], axis=1),
            cells_of(i, at), LANES, preferred_element_type=F32,
        )

    near, far = [0] + PLANE_ORDER[:3:-1], PLANE_ORDER[:4]
    for d in near[1:]:
        spread_copy(d).wait_recv()
    for i in range(CHUNKS):
        @pl.when(z >= 0)
        def _():
            partial[i] = scores_with(i, near)

    for d in far:
        spread_copy(d).wait_recv()
    for i in range(CHUNKS):
        chunk(1, i, lambda i: partial[i] + scores_with(i, far))
    join(1)
    gram_start(1)
    product_start(1)
    gram_middle(1)
    block = product_middle(1, 0)
    turned = jnp.transpose(jnp.concatenate([block, block], axis=0))
    lane_half = lax.broadcasted_iota(jnp.int32, (8, 2 * K), 1) < K
    for zz in range(NZ):
        pieces[zz] = jnp.where(lane_half, turned[16 * zz : 16 * zz + 8], turned[16 * zz + 8 : 16 * zz + 16])

    def piece_copy(d):
        peer = on_z(d, core)
        return copy_of(pieces.at[peer[2]], pieces_in.at[d], PER_ROUND + DEEP + d, peer)

    for d in Z_ORDER:
        piece_copy(d).start()
    gram_end(1)
    for d in Z_ORDER:
        piece_copy(d).wait_recv()
    piece = pieces[z]
    for d in range(1, NZ):
        piece = piece + pieces_in[d]
    piece_ref[...] = piece

    left(0)
    for h in range(HALVES[0]):
        for d in Z_ORDER:
            whole_copy(h, d).wait_send()
    for d in PLANE_ORDER:
        spread_copy(d).wait_send()
    left(1)
    for d in Z_ORDER:
        piece_copy(d).wait_send()


def local(tiles, tile_row, tile_col, tile_count, start_basis):
    vmem = pl.BlockSpec(memory_space=pltpu.VMEM)
    anywhere = pl.BlockSpec(memory_space=pltpu.HBM)
    parts = pl.pallas_call(
        kernel,
        out_shape=(
            pltpu.VMEM((K, 4 * K), BF16),
            pltpu.VMEM((2 * K, CELLS), BF16),
            pltpu.VMEM((8, TILE), F32),
        ),
        in_specs=[anywhere] * 5,
        out_specs=(vmem, vmem, vmem),
        scratch_shapes=[
            pltpu.VMEM((2, 1, SLOTS), jnp.int32),
            pltpu.VMEM((1, 1), jnp.int32),
            pltpu.VMEM((1, ROW_BLOCKS * COL_BLOCKS), jnp.int32),
            pltpu.SMEM((1, ROW_BLOCKS * COL_BLOCKS), jnp.int32),
            pltpu.VMEM((SLOTS + 1, TILE, TILE), BF16),
            pltpu.VMEM((COL_BLOCKS, CELLS, TILE), BF16),
            pltpu.VMEM((K, GENES), BF16),
            pltpu.VMEM((2, CHUNKS, K, CHUNK), F32),
            pltpu.VMEM((2, CHUNKS, K, CHUNK), F32),
            pltpu.VMEM((2, PLANE, K, TILE), F32),
            pltpu.VMEM((2, PLANE, K, TILE), F32),
            pltpu.VMEM((NZ, K, TILE), F32),
            pltpu.VMEM((NZ, 8, TILE), F32),
            pltpu.VMEM((NZ, 8, TILE), F32),
            pltpu.VMEM((2, 24, 2 * K), F32),
            pltpu.VMEM((2, PLANE, 24, 2 * K), F32),
            pltpu.VMEM((2, NZ, 24, 2 * K), F32),
            pltpu.VMEM((24, 2 * K), F32),
            pltpu.VMEM((PLANE, K, TILE), BF16),
            pltpu.VMEM((CHUNKS, K, CHUNK), F32),
            pltpu.SemaphoreType.DMA((5 + LOADS,)),
            pltpu.SemaphoreType.DMA((MESSAGES,)),
            pltpu.SemaphoreType.DMA((MESSAGES,)),
        ],
        compiler_params=pltpu.CompilerParams(collective_id=0, has_side_effects=True),
    )(tile_row, tile_col, tile_count, tiles[0], start_basis)
    basis, loadings = pl.pallas_call(
        finish,
        out_shape=(
            jax.ShapeDtypeStruct((K, CELLS), BF16),
            jax.ShapeDtypeStruct((GENES // (PLANE * NZ), K), F32),
        ),
        in_specs=[vmem] * 3,
        out_specs=(vmem, vmem),
    )(*(pltpu.with_memory_space_constraint(part, pltpu.VMEM) for part in parts))
    return basis, loadings.T


def solution(mesh):
    finer = Mesh(
        mesh.devices.reshape(NY, NX, NZ, mesh.shape["gene"]), ("cell_0", "cell_1", "cell_2", "gene")
    )
    return jax.shard_map(
        local,
        mesh=finer,
        in_specs=(
            P("gene", CELL, None, None),
            P("gene", CELL),
            P("gene", CELL),
            P("gene", CELL),
            P(None, "gene"),
        ),
        out_specs=(P(None, CELL), P(None, GENE_CELL)),
        check_vma=False,
    )
```

```python
import jax
import jax.numpy as jnp
from jax import lax
from jax.experimental import pallas as pl
from jax.experimental.pallas import tpu as pltpu
from jax.sharding import Mesh
from jax.sharding import PartitionSpec as P

K = 64
TILE = 128
ROW_BLOCKS = 8
COL_BLOCKS = 16
SLOTS = 64
CELLS = ROW_BLOCKS * TILE
GENES = COL_BLOCKS * TILE
NY, NX, NZ = 4, 4, 8
PLANE = NY * NX
CHUNKS = 2
CHUNK = CELLS // CHUNKS
PAIRS = COL_BLOCKS // 2
TOTAL_CELLS = PLANE * NZ * CELLS
CELL = ("cell_0", "cell_1", "cell_2")
GENE_CELL = ("gene", "cell_0", "cell_1", "cell_2")
MESH = pl.DeviceIdType.MESH
F32 = jnp.float32
BF16 = jnp.bfloat16
LANES = (((1,), (1,)), ((), ()))

PAIR, ACROSS, DEEP, GACROSS, GDEEP = 0, 2, 34, 50, 66
PER_ROUND = 82
LOADS = 1
HALVES = (2, 1)
SPREAD = 2 * PER_ROUND
MESSAGES = SPREAD + PLANE


def hops(d):
    dy, dx = d // NX, d % NX
    return min(dy, NY - dy) + min(dx, NX - dx)


PLANE_ORDER = sorted(range(1, PLANE), key=lambda d: -hops(d))
Z_ORDER = sorted(range(1, NZ), key=lambda d: -min(d, NZ - d))


def split(value):
    high = value.astype(BF16)
    return high, (value - high.astype(F32)).astype(BF16)


def spread_lane(value, at):
    return jnp.broadcast_to(value[:, at : at + 1], value.shape)


def pack(twice):
    quarter = lax.broadcasted_iota(jnp.int32, (8, 2 * K), 1) // 32
    ahead, back = pltpu.roll(twice, 32, 1), pltpu.roll(twice, 96, 1)

    def joined(row, sources):
        value = sources[0][row : row + 8]
        for k in range(1, 4):
            value = jnp.where(quarter == k, sources[k][row + 8 * k : row + 8 * k + 8], value)
        return value

    return jnp.concatenate(
        [joined(0, (twice, ahead) * 2), joined(32, (twice, ahead) * 2), joined(32, (back, twice) * 2)], axis=0
    )


def invert(packed):
    lane = lax.broadcasted_iota(jnp.int32, (8, 2 * K), 1)
    inner = lax.broadcasted_iota(jnp.int32, (8, 2 * K), 0)

    def moved(block, shift):
        return pltpu.roll(block, shift % 128, 1) if shift % 128 else block

    left = [moved(packed[8 * (p // 4) : 8 * (p // 4) + 8], -32 * (p % 4)) for p in range(8)]
    under = [jnp.where(lane < 32, left[4 + k], moved(packed[16:24], 32 - 32 * k)) for k in range(4)]
    turned = jnp.transpose(jnp.concatenate((left[:4] + under) * 2, axis=0))
    parts = []
    for p in range(8):
        side = jnp.where(lane < 32, left[p], turned[8 * p : 8 * p + 8]) if p < 4 else under[p - 4]
        eye = (lane == inner + (K + 8 * p)).astype(F32)
        parts.append(jnp.where(lane < K, side, eye))
    out = []
    for p in range(8):
        block = parts[p]
        wide = [spread_lane(block, 8 * p + j) for j in range(8)]
        e = [[None] * 8 for _ in range(8)]
        for s in range(8):
            for j in range(s + 1):
                e[s][j] = jnp.broadcast_to(wide[j][s : s + 1, :], (8, 2 * K))
        rows = [jnp.broadcast_to(block[s : s + 1, :], (8, 2 * K)) for s in range(8)]
        lead = [
            [spread_lane(parts[q], 8 * p + j) for j in range(8)]
            for q in range(p + 1, 8)
        ]
        done = jnp.zeros((8, 2 * K), F32)
        for j in range(8):
            over = 1.0 / e[j][j]
            m = [e[s][j] * over for s in range(j + 1, 8)]
            for s in range(j + 1, 8):
                for t in range(j + 1, s + 1):
                    e[s][t] = e[s][t] - m[s - j - 1] * e[t][j]
            for s in range(j + 1, 8):
                rows[s] = rows[s] - m[s - j - 1] * rows[j]
            done = jnp.where(inner == j, rows[j] * lax.rsqrt(e[j][j]), done)
            for q in range(p + 1, 8):
                mine = lead[q - p - 1]
                for t in range(j + 1, 8):
                    mine[t] = mine[t] - mine[j] * m[t - j - 1]
                parts[q] = parts[q] - (mine[j] * over) * rows[j]
        out.append(done)
    return jnp.concatenate(out, axis=0)[:, K:]


def finish(lower_ref, both_ref, piece_ref, basis_ref, loadings_ref):
    ortho = jnp.dot(
        lower_ref[...], jnp.concatenate([both_ref[...], both_ref[...]], axis=0), preferred_element_type=F32
    )
    basis_ref[...] = (ortho * jnp.sqrt(F32(TOTAL_CELLS))).astype(BF16)
    piece = piece_ref[...]
    high, low = split(jnp.concatenate([piece[:, :K], piece[:, K:]], axis=0))
    loadings_ref[...] = lax.dot_general(
        jnp.concatenate([high, low, high, low], axis=1), lower_ref[...], LANES, preferred_element_type=F32
    )


def kernel(
    row_any, col_any, count_any, tiles_any, start_any, lower_ref, both, piece_ref,
    places, count, inverse_v, inverse, tiles, x_ref, xt_ref, start, own, other, product, across, deep_in, pieces, pieces_in,
    gram, gacross, gdeep, gram_sum, mid, partial, load_sem, send_sem, recv_sem,
):
    y, x, z = (lax.axis_index(name) for name in CELL)
    core = lax.axis_index("gene")
    other_core = 1 - core
    here = NX * y + x

    def in_plane(d):
        return (lax.rem(y + d // NX, NY), lax.rem(x + d % NX, NX), z, core)

    def on_z(d, which):
        return (y, x, lax.rem(z + d, NZ), which)

    partner = (y, x, z, other_core)
    loads = [
        pltpu.make_async_copy(row_any, places.at[0], load_sem.at[0]),
        pltpu.make_async_copy(col_any, places.at[1], load_sem.at[1]),
        pltpu.make_async_copy(count_any, count, load_sem.at[2]),
        pltpu.make_async_copy(start_any, start, load_sem.at[3]),
    ]
    for n in range(LOADS):
        rows = pl.ds(n * SLOTS // LOADS, SLOTS // LOADS)
        loads.append(pltpu.make_async_copy(tiles_any.at[rows], tiles.at[rows], load_sem.at[5 + n]))
    for load in loads:
        load.start()

    barrier = pltpu.get_barrier_semaphore()
    peers = [partner] + [in_plane(d) for d in range(1, PLANE)]
    peers += [on_z(d, which) for which in (core, other_core) for d in Z_ORDER]
    for peer in peers:
        pl.semaphore_signal(barrier, inc=1, device_id=peer, device_id_type=MESH)

    tiles[SLOTS] = jnp.zeros((TILE, TILE), BF16)
    for load in loads[:3]:
        load.wait()
    lane = lax.broadcasted_iota(jnp.int32, (1, SLOTS), 1)
    place = jnp.where(lane < count[...], places[0] * COL_BLOCKS + places[1], ROW_BLOCKS * COL_BLOCKS)
    turned = jnp.transpose(jnp.broadcast_to(jnp.concatenate([place, place], axis=1), (TILE, TILE)))[:SLOTS]
    slot = lax.broadcasted_iota(jnp.int32, (SLOTS, TILE), 0)
    spot = lax.broadcasted_iota(jnp.int32, (SLOTS, TILE), 1)
    inverse_v[...] = jnp.min(jnp.where(turned == spot, slot, SLOTS), axis=0, keepdims=True)
    lookup = pltpu.make_async_copy(inverse_v, inverse, load_sem.at[4])
    lookup.start()
    for load in loads[3:]:
        load.wait()
    lookup.wait()

    def copy_of(src, dst, number, peer):
        return pltpu.make_async_remote_copy(
            src_ref=src, dst_ref=dst, send_sem=send_sem.at[number], recv_sem=recv_sem.at[number],
            device_id=peer, device_id_type=MESH,
        )

    def pair_copy(r, i):
        return copy_of(own.at[r, i], other.at[r, i], r * PER_ROUND + PAIR + i, partner)

    def build(i):
        for k in range(CHUNK // TILE):
            row = i * CHUNK + k * TILE
            for c in range(COL_BLOCKS):
                x_ref[c, row : row + TILE] = tiles[inverse[0, row // TILE * COL_BLOCKS + c]]

    def cells_of(i, columns):
        return jnp.concatenate([x_ref[n, i * CHUNK : (i + 1) * CHUNK] for n in columns], axis=1)

    def chunk(r, i, scores_of):
        @pl.when(z >= 0)
        def _():
            if r == 1 and i > 0:
                pair_copy(r, i - 1).start()
            if r == 0 and i + 1 < CHUNKS:
                build(i + 1)
            own[r, i] = scores_of(i)

    def join(r):
        if r == 0:
            pl.semaphore_wait(barrier, len(peers))
            for i in range(CHUNKS - 1):
                pair_copy(r, i).start()
        pair_copy(r, CHUNKS - 1).start()
        for i in range(CHUNKS):
            pair_copy(r, i).wait_recv()
            high, low = split(own[r, i] + other[r, i])
            both[:K, i * CHUNK : (i + 1) * CHUNK] = high
            both[K:, i * CHUNK : (i + 1) * CHUNK] = low

    def gram_across(r, d):
        return copy_of(gram.at[r], gacross.at[r, here], r * PER_ROUND + GACROSS + d, in_plane(d))

    def gram_deep(r, d, which):
        number = r * PER_ROUND + GDEEP + 8 * (1 - which) + d
        return copy_of(gdeep.at[r, z], gdeep.at[r, z], number, on_z(d, which))

    def gram_start(r):
        @pl.when(core == 1)
        def _():
            square = lax.dot_general(both[...], both[...], LANES, preferred_element_type=F32)
            square = square[:K] + square[K:]
            square = square + pltpu.roll(square, K, 1)
            packed = pack(square)
            gram[r] = packed
            gacross[r, here] = packed
            for d in PLANE_ORDER:
                gram_across(r, d).start()

    def gram_middle(r):
        @pl.when(core == 1)
        def _():
            for d in PLANE_ORDER:
                gram_across(r, d).wait_recv()
            total = gacross[r, 0]
            for n in range(1, PLANE):
                total = total + gacross[r, n]
            gdeep[r, z] = total
            for d in Z_ORDER:
                gram_deep(r, d, 1).start()
                if r == 1:
                    gram_deep(r, d, 0).start()
            if r == 1:
                gram_deep(r, 0, 0).start()

    def gram_pair():
        return copy_of(gram_sum, gram_sum, GDEEP + NZ, partner)

    def gram_end(r):
        @pl.when(core == 1)
        def _():
            for d in Z_ORDER:
                gram_deep(r, d, 1).wait_recv()
            if r == 0:
                total = gdeep[r, 0]
                for zz in range(1, NZ):
                    total = total + gdeep[r, zz]
                gram_sum[...] = total
                gram_pair().start()

        @pl.when(core == 0)
        def _():
            if r == 0:
                gram_pair().wait_recv()
            else:
                for d in range(NZ):
                    gram_deep(r, d, 0).wait_recv()

        @pl.when(z >= 0)
        def _():
            if r == 0:
                total = gram_sum[...]
            else:
                total = gdeep[r, 0]
                for zz in range(1, NZ):
                    total = total + gdeep[r, zz]
            high, low = split(invert(total))
            lower_ref[...] = jnp.concatenate([high, high, low, low], axis=1)

    def product_copy(r, h, n, d, peer):
        rows = pl.ds(h * K // HALVES[r], K // HALVES[r])
        number = r * PER_ROUND + ACROSS + PLANE * h + d
        return copy_of(product.at[r, n, rows], across.at[r, d, rows], number, peer)

    def product_start(r):
        def send(h, dy, dx):
            if dy or dx:
                yy, xx = lax.rem(y + dy, NY), lax.rem(x + dx, NX)
                product_copy(r, h, NX * yy + xx, NX * dy + dx, (yy, xx, z, core)).start()

        for dy in (2, 1, 3, 0):
            n = NX * lax.rem(y + dy, NY)

            @pl.when(z >= 0)
            def _():
                doubled = jnp.dot(
                    both[...], jnp.concatenate([x_ref[n + k] for k in range(NX)], axis=1), preferred_element_type=F32
                )
                summed = doubled[:K] + doubled[K:]
                for k in range(NX):
                    product[r, n + k] = summed[:, k * TILE : (k + 1) * TILE]
                for dx in (2, 1, 3, 0):
                    pl.when(core >= r)(lambda dy=dy, dx=dx: send(0, dy, dx))

        @pl.when(core < r)
        def _():
            for d in PLANE_ORDER:
                send(0, d // NX, d % NX)

        for h in range(1, HALVES[r]):
            for d in PLANE_ORDER:
                send(h, d // NX, d % NX)

    def product_middle(r, h):
        for d in PLANE_ORDER:
            product_copy(r, h, 0, d, in_plane(d)).wait_recv()
        rows = slice(h * K // HALVES[r], (h + 1) * K // HALVES[r])
        total = product[r, here, rows]
        for d in range(1, PLANE):
            total = total + across[r, d, rows]
        return total

    def left(r):
        for i in range(CHUNKS):
            pair_copy(r, i).wait_send()
        for h in range(HALVES[r]):
            for d in PLANE_ORDER:
                product_copy(r, h, 0, d, in_plane(d)).wait_send()

        @pl.when(core == 1)
        def _():
            for d in PLANE_ORDER:
                gram_across(r, d).wait_send()
            for d in Z_ORDER:
                gram_deep(r, d, 1).wait_send()
            if r == 0:
                gram_pair().wait_send()
            else:
                for d in range(NZ):
                    gram_deep(r, d, 0).wait_send()

    def turn_over():
        def column(c, carry):
            for i in range(CHUNKS):
                strip = jnp.concatenate(
                    [jnp.transpose(x_ref[c, i * CHUNK + k * TILE : i * CHUNK + (k + 1) * TILE]) for k in range(CHUNK // TILE)],
                    axis=1,
                )
                xt_ref[i, c] = strip
            return carry

        lax.fori_loop(0, COL_BLOCKS, column, 0)

    build(0)
    for i in range(CHUNKS):
        chunk(
            0, i, lambda i: lax.dot_general(
                start[...], cells_of(i, range(COL_BLOCKS)), LANES, preferred_element_type=F32
            ),
        )
    join(0)
    gram_start(0)
    product_start(0)
    turn_over()
    gram_middle(0)
    def whole_copy(h, d):
        rows = pl.ds(h * K // HALVES[0], K // HALVES[0])
        return copy_of(deep_in.at[z, rows], deep_in.at[z, rows], DEEP + NZ * h + d, on_z(d, core))

    for h in range(HALVES[0]):
        deep_in[z, h * K // HALVES[0] : (h + 1) * K // HALVES[0]] = product_middle(0, h)
        for d in Z_ORDER:
            whole_copy(h, d).start()
    gram_end(0)
    for h in range(HALVES[0]):
        for d in Z_ORDER:
            whole_copy(h, d).wait_recv()
    total = deep_in[0]
    for zz in range(1, NZ):
        total = total + deep_in[zz]
    high, low = split(total)
    middle = jnp.dot(
        lower_ref[...], jnp.concatenate([high, low, high, low], axis=0), preferred_element_type=F32
    )
    mid[here] = middle.astype(BF16)

    def spread_copy(d):
        return copy_of(mid.at[here], mid.at[here], SPREAD + d, in_plane(d))

    for d in PLANE_ORDER:
        spread_copy(d).start()
    def scores_with(i, offsets):
        at = [NX * lax.rem(y + NY - d // NX, NY) + lax.rem(x + NX - d % NX, NX) for d in offsets]
        return lax.dot_general(
            jnp.concatenate([mid[n] for n in at], axis=1),
            jnp.concatenate([xt_ref[i, n] for n in at], axis=0), (((1,), (0,)), ((), ())),
            preferred_element_type=F32,
        )

    near, far = [0] + PLANE_ORDER[:3:-1], PLANE_ORDER[:4]
    for d in near[1:]:
        spread_copy(d).wait_recv()
    for i in range(CHUNKS):
        @pl.when(z >= 0)
        def _():
            partial[i] = scores_with(i, near)

    for d in far:
        spread_copy(d).wait_recv()
    for i in range(CHUNKS):
        chunk(1, i, lambda i: partial[i] + scores_with(i, far))
    join(1)
    gram_start(1)
    product_start(1)
    gram_middle(1)
    block = product_middle(1, 0)
    turned = jnp.transpose(jnp.concatenate([block, block], axis=0))
    lane_half = lax.broadcasted_iota(jnp.int32, (8, 2 * K), 1) < K
    for zz in range(NZ):
        pieces[zz] = jnp.where(lane_half, turned[16 * zz : 16 * zz + 8], turned[16 * zz + 8 : 16 * zz + 16])

    def piece_copy(d):
        peer = on_z(d, core)
        return copy_of(pieces.at[peer[2]], pieces_in.at[d], PER_ROUND + DEEP + d, peer)

    for d in Z_ORDER:
        piece_copy(d).start()
    gram_end(1)
    for d in Z_ORDER:
        piece_copy(d).wait_recv()
    piece = pieces[z]
    for d in range(1, NZ):
        piece = piece + pieces_in[d]
    piece_ref[...] = piece

    left(0)
    for h in range(HALVES[0]):
        for d in Z_ORDER:
            whole_copy(h, d).wait_send()
    for d in PLANE_ORDER:
        spread_copy(d).wait_send()
    left(1)
    for d in Z_ORDER:
        piece_copy(d).wait_send()


def local(tiles, tile_row, tile_col, tile_count, start_basis):
    vmem = pl.BlockSpec(memory_space=pltpu.VMEM)
    anywhere = pl.BlockSpec(memory_space=pltpu.HBM)
    parts = pl.pallas_call(
        kernel,
        out_shape=(
            pltpu.VMEM((K, 4 * K), BF16),
            pltpu.VMEM((2 * K, CELLS), BF16),
            pltpu.VMEM((8, TILE), F32),
        ),
        in_specs=[anywhere] * 5,
        out_specs=(vmem, vmem, vmem),
        scratch_shapes=[
            pltpu.VMEM((2, 1, SLOTS), jnp.int32),
            pltpu.VMEM((1, 1), jnp.int32),
            pltpu.VMEM((1, ROW_BLOCKS * COL_BLOCKS), jnp.int32),
            pltpu.SMEM((1, ROW_BLOCKS * COL_BLOCKS), jnp.int32),
            pltpu.VMEM((SLOTS + 1, TILE, TILE), BF16),
            pltpu.VMEM((COL_BLOCKS, CELLS, TILE), BF16),
            pltpu.VMEM((CHUNKS, COL_BLOCKS, TILE, CHUNK), BF16),
            pltpu.VMEM((K, GENES), BF16),
            pltpu.VMEM((2, CHUNKS, K, CHUNK), F32),
            pltpu.VMEM((2, CHUNKS, K, CHUNK), F32),
            pltpu.VMEM((2, PLANE, K, TILE), F32),
            pltpu.VMEM((2, PLANE, K, TILE), F32),
            pltpu.VMEM((NZ, K, TILE), F32),
            pltpu.VMEM((NZ, 8, TILE), F32),
            pltpu.VMEM((NZ, 8, TILE), F32),
            pltpu.VMEM((2, 24, 2 * K), F32),
            pltpu.VMEM((2, PLANE, 24, 2 * K), F32),
            pltpu.VMEM((2, NZ, 24, 2 * K), F32),
            pltpu.VMEM((24, 2 * K), F32),
            pltpu.VMEM((PLANE, K, TILE), BF16),
            pltpu.VMEM((CHUNKS, K, CHUNK), F32),
            pltpu.SemaphoreType.DMA((5 + LOADS,)),
            pltpu.SemaphoreType.DMA((MESSAGES,)),
            pltpu.SemaphoreType.DMA((MESSAGES,)),
        ],
        compiler_params=pltpu.CompilerParams(collective_id=0, has_side_effects=True),
    )(tile_row, tile_col, tile_count, tiles[0], start_basis)
    basis, loadings = pl.pallas_call(
        finish,
        out_shape=(
            jax.ShapeDtypeStruct((K, CELLS), BF16),
            jax.ShapeDtypeStruct((GENES // (PLANE * NZ), K), F32),
        ),
        in_specs=[vmem] * 3,
        out_specs=(vmem, vmem),
    )(*(pltpu.with_memory_space_constraint(part, pltpu.VMEM) for part in parts))
    return basis, loadings.T


def solution(mesh):
    finer = Mesh(
        mesh.devices.reshape(NY, NX, NZ, mesh.shape["gene"]), ("cell_0", "cell_1", "cell_2", "gene")
    )
    return jax.shard_map(
        local,
        mesh=finer,
        in_specs=(
            P("gene", CELL, None, None),
            P("gene", CELL),
            P("gene", CELL),
            P("gene", CELL),
            P(None, "gene"),
        ),
        out_specs=(P(None, CELL), P(None, GENE_CELL)),
        check_vma=False,
    )
```

```python
import jax
import jax.numpy as jnp
from jax import lax
from jax.experimental import pallas as pl
from jax.experimental.pallas import tpu as pltpu
from jax.sharding import Mesh
from jax.sharding import PartitionSpec as P

K = 64
TILE = 128
ROW_BLOCKS = 8
COL_BLOCKS = 16
SLOTS = 64
CELLS = ROW_BLOCKS * TILE
GENES = COL_BLOCKS * TILE
NY, NX, NZ = 4, 4, 8
PLANE = NY * NX
CHUNKS = 2
CHUNK = CELLS // CHUNKS
PAIRS = COL_BLOCKS // 2
TOTAL_CELLS = PLANE * NZ * CELLS
CELL = ("cell_0", "cell_1", "cell_2")
GENE_CELL = ("gene", "cell_0", "cell_1", "cell_2")
MESH = pl.DeviceIdType.MESH
F32 = jnp.float32
BF16 = jnp.bfloat16
LANES = (((1,), (1,)), ((), ()))

PAIR, ACROSS, DEEP, GACROSS, GDEEP = 0, 2, 34, 50, 66
PER_ROUND = 82
LOADS = 1
HALVES = (2, 1)
SPREAD = 2 * PER_ROUND
MESSAGES = SPREAD + PLANE


def hops(d):
    dy, dx = d // NX, d % NX
    return min(dy, NY - dy) + min(dx, NX - dx)


PLANE_ORDER = sorted(range(1, PLANE), key=lambda d: -hops(d))
Z_ORDER = sorted(range(1, NZ), key=lambda d: -min(d, NZ - d))


def split(value):
    high = value.astype(BF16)
    return high, (value - high.astype(F32)).astype(BF16)


def spread_lane(value, at):
    return jnp.broadcast_to(value[:, at : at + 1], value.shape)


def pack(twice):
    quarter = lax.broadcasted_iota(jnp.int32, (8, 2 * K), 1) // 32
    ahead, back = pltpu.roll(twice, 32, 1), pltpu.roll(twice, 96, 1)

    def joined(row, sources):
        value = sources[0][row : row + 8]
        for k in range(1, 4):
            value = jnp.where(quarter == k, sources[k][row + 8 * k : row + 8 * k + 8], value)
        return value

    return jnp.concatenate(
        [joined(0, (twice, ahead) * 2), joined(32, (twice, ahead) * 2), joined(32, (back, twice) * 2)], axis=0
    )


def invert(packed):
    lane = lax.broadcasted_iota(jnp.int32, (8, 2 * K), 1)
    inner = lax.broadcasted_iota(jnp.int32, (8, 2 * K), 0)

    def moved(block, shift):
        return pltpu.roll(block, shift % 128, 1) if shift % 128 else block

    left = [moved(packed[8 * (p // 4) : 8 * (p // 4) + 8], -32 * (p % 4)) for p in range(8)]
    under = [jnp.where(lane < 32, left[4 + k], moved(packed[16:24], 32 - 32 * k)) for k in range(4)]
    turned = jnp.transpose(jnp.concatenate((left[:4] + under) * 2, axis=0))
    parts = []
    for p in range(8):
        side = jnp.where(lane < 32, left[p], turned[8 * p : 8 * p + 8]) if p < 4 else under[p - 4]
        eye = (lane == inner + (K + 8 * p)).astype(F32)
        parts.append(jnp.where(lane < K, side, eye))
    out = []
    for p in range(8):
        block = parts[p]
        wide = [spread_lane(block, 8 * p + j) for j in range(8)]
        e = [[None] * 8 for _ in range(8)]
        for s in range(8):
            for j in range(s + 1):
                e[s][j] = jnp.broadcast_to(wide[j][s : s + 1, :], (8, 2 * K))
        rows = [jnp.broadcast_to(block[s : s + 1, :], (8, 2 * K)) for s in range(8)]
        lead = [
            [spread_lane(parts[q], 8 * p + j) for j in range(8)]
            for q in range(p + 1, 8)
        ]
        done = jnp.zeros((8, 2 * K), F32)
        for j in range(8):
            over = 1.0 / e[j][j]
            m = [e[s][j] * over for s in range(j + 1, 8)]
            for s in range(j + 1, 8):
                for t in range(j + 1, s + 1):
                    e[s][t] = e[s][t] - m[s - j - 1] * e[t][j]
            for s in range(j + 1, 8):
                rows[s] = rows[s] - m[s - j - 1] * rows[j]
            done = jnp.where(inner == j, rows[j] * lax.rsqrt(e[j][j]), done)
            for q in range(p + 1, 8):
                mine = lead[q - p - 1]
                for t in range(j + 1, 8):
                    mine[t] = mine[t] - mine[j] * m[t - j - 1]
                parts[q] = parts[q] - (mine[j] * over) * rows[j]
        out.append(done)
    return jnp.concatenate(out, axis=0)[:, K:]


def finish(lower_ref, both_ref, piece_ref, basis_ref, loadings_ref):
    ortho = jnp.dot(
        lower_ref[...], jnp.concatenate([both_ref[...], both_ref[...]], axis=0), preferred_element_type=F32
    )
    basis_ref[...] = (ortho * jnp.sqrt(F32(TOTAL_CELLS))).astype(BF16)
    piece = piece_ref[...]
    high, low = split(jnp.concatenate([piece[:, :K], piece[:, K:]], axis=0))
    loadings_ref[...] = lax.dot_general(
        jnp.concatenate([high, low, high, low], axis=1), lower_ref[...], LANES, preferred_element_type=F32
    )


def kernel(
    row_any, col_any, count_any, tiles_any, start_any, lower_ref, both, piece_ref,
    places, count, inverse_v, inverse, tiles, x_ref, xt_ref, start, own, other, product, across, deep_in, pieces, pieces_in,
    gram, gacross, gdeep, gram_sum, mid, partial, load_sem, send_sem, recv_sem,
):
    y, x, z = (lax.axis_index(name) for name in CELL)
    core = lax.axis_index("gene")
    other_core = 1 - core
    here = NX * y + x

    def in_plane(d):
        return (lax.rem(y + d // NX, NY), lax.rem(x + d % NX, NX), z, core)

    def on_z(d, which):
        return (y, x, lax.rem(z + d, NZ), which)

    partner = (y, x, z, other_core)
    loads = [
        pltpu.make_async_copy(row_any, places.at[0], load_sem.at[0]),
        pltpu.make_async_copy(col_any, places.at[1], load_sem.at[1]),
        pltpu.make_async_copy(count_any, count, load_sem.at[2]),
        pltpu.make_async_copy(start_any, start, load_sem.at[3]),
    ]
    for n in range(LOADS):
        rows = pl.ds(n * SLOTS // LOADS, SLOTS // LOADS)
        loads.append(pltpu.make_async_copy(tiles_any.at[rows], tiles.at[rows], load_sem.at[5 + n]))
    for load in loads:
        load.start()

    barrier = pltpu.get_barrier_semaphore()
    peers = [partner] + [in_plane(d) for d in range(1, PLANE)]
    peers += [on_z(d, which) for which in (core, other_core) for d in Z_ORDER]
    for peer in peers:
        pl.semaphore_signal(barrier, inc=1, device_id=peer, device_id_type=MESH)

    tiles[SLOTS] = jnp.zeros((TILE, TILE), BF16)
    for load in loads[:3]:
        load.wait()
    lane = lax.broadcasted_iota(jnp.int32, (1, SLOTS), 1)
    place = jnp.where(lane < count[...], places[0] * COL_BLOCKS + places[1], ROW_BLOCKS * COL_BLOCKS)
    turned = jnp.transpose(jnp.broadcast_to(jnp.concatenate([place, place], axis=1), (TILE, TILE)))[:SLOTS]
    slot = lax.broadcasted_iota(jnp.int32, (SLOTS, TILE), 0)
    spot = lax.broadcasted_iota(jnp.int32, (SLOTS, TILE), 1)
    inverse_v[...] = jnp.min(jnp.where(turned == spot, slot, SLOTS), axis=0, keepdims=True)
    lookup = pltpu.make_async_copy(inverse_v, inverse, load_sem.at[4])
    lookup.start()
    for load in loads[3:]:
        load.wait()
    lookup.wait()

    def copy_of(src, dst, number, peer):
        return pltpu.make_async_remote_copy(
            src_ref=src, dst_ref=dst, send_sem=send_sem.at[number], recv_sem=recv_sem.at[number],
            device_id=peer, device_id_type=MESH,
        )

    def pair_copy(r, i):
        return copy_of(own.at[r, i], other.at[r, i], r * PER_ROUND + PAIR + i, partner)

    def build(i):
        for k in range(CHUNK // TILE):
            row = i * CHUNK + k * TILE
            for c in range(COL_BLOCKS):
                x_ref[c, row : row + TILE] = tiles[inverse[0, row // TILE * COL_BLOCKS + c]]

    def cells_of(i, columns):
        return jnp.concatenate([x_ref[n, i * CHUNK : (i + 1) * CHUNK] for n in columns], axis=1)

    def chunk(r, i, scores_of):
        @pl.when(z >= 0)
        def _():
            if r == 1 and i > 0:
                pair_copy(r, i - 1).start()
            if r == 0 and i + 1 < CHUNKS:
                build(i + 1)
            own[r, i] = scores_of(i)

    def join(r):
        if r == 0:
            pl.semaphore_wait(barrier, len(peers))
            for i in range(CHUNKS - 1):
                pair_copy(r, i).start()
        pair_copy(r, CHUNKS - 1).start()
        for i in range(CHUNKS):
            pair_copy(r, i).wait_recv()
            high, low = split(own[r, i] + other[r, i])
            both[:K, i * CHUNK : (i + 1) * CHUNK] = high
            both[K:, i * CHUNK : (i + 1) * CHUNK] = low

    def gram_across(r, d):
        return copy_of(gram.at[r], gacross.at[r, here], r * PER_ROUND + GACROSS + d, in_plane(d))

    def gram_deep(r, d, which):
        number = r * PER_ROUND + GDEEP + 8 * (1 - which) + d
        return copy_of(gdeep.at[r, z], gdeep.at[r, z], number, on_z(d, which))

    def gram_start(r):
        @pl.when(core == 1)
        def _():
            halves = [both[:, i * CHUNK : (i + 1) * CHUNK] for i in range(CHUNKS)]
            squares = [lax.dot_general(half, half, LANES, preferred_element_type=F32) for half in halves]
            square = sum(part[:K] + part[K:] for part in squares)
            square = square + pltpu.roll(square, K, 1)
            packed = pack(square)
            gram[r] = packed
            gacross[r, here] = packed
            for d in PLANE_ORDER:
                gram_across(r, d).start()

    def gram_middle(r):
        @pl.when(core == 1)
        def _():
            for d in PLANE_ORDER:
                gram_across(r, d).wait_recv()
            total = gacross[r, 0]
            for n in range(1, PLANE):
                total = total + gacross[r, n]
            gdeep[r, z] = total
            for d in Z_ORDER:
                gram_deep(r, d, 1).start()
                if r == 1:
                    gram_deep(r, d, 0).start()
            if r == 1:
                gram_deep(r, 0, 0).start()

    def gram_pair():
        return copy_of(gram_sum, gram_sum, GDEEP + NZ, partner)

    def gram_end(r):
        @pl.when(core == 1)
        def _():
            for d in Z_ORDER:
                gram_deep(r, d, 1).wait_recv()
            if r == 0:
                total = gdeep[r, 0]
                for zz in range(1, NZ):
                    total = total + gdeep[r, zz]
                gram_sum[...] = total
                gram_pair().start()

        @pl.when(core == 0)
        def _():
            if r == 0:
                gram_pair().wait_recv()
            else:
                for d in range(NZ):
                    gram_deep(r, d, 0).wait_recv()

        @pl.when(z >= 0)
        def _():
            if r == 0:
                total = gram_sum[...]
            else:
                total = gdeep[r, 0]
                for zz in range(1, NZ):
                    total = total + gdeep[r, zz]
            high, low = split(invert(total))
            lower_ref[...] = jnp.concatenate([high, high, low, low], axis=1)

    def product_copy(r, h, n, d, peer):
        rows = pl.ds(h * K // HALVES[r], K // HALVES[r])
        number = r * PER_ROUND + ACROSS + PLANE * h + d
        return copy_of(product.at[r, n, rows], across.at[r, d, rows], number, peer)

    def product_start(r):
        def send(h, dy, dx):
            if dy or dx:
                yy, xx = lax.rem(y + dy, NY), lax.rem(x + dx, NX)
                product_copy(r, h, NX * yy + xx, NX * dy + dx, (yy, xx, z, core)).start()

        for dy in (2, 1, 3, 0):
            n = NX * lax.rem(y + dy, NY)

            @pl.when(z >= 0)
            def _():
                doubled = jnp.dot(
                    both[...], jnp.concatenate([x_ref[n + k] for k in range(NX)], axis=1), preferred_element_type=F32
                )
                summed = doubled[:K] + doubled[K:]
                for k in range(NX):
                    product[r, n + k] = summed[:, k * TILE : (k + 1) * TILE]
                for dx in (2, 1, 3, 0):
                    pl.when(core >= r)(lambda dy=dy, dx=dx: send(0, dy, dx))

        @pl.when(core < r)
        def _():
            for d in PLANE_ORDER:
                send(0, d // NX, d % NX)

        for h in range(1, HALVES[r]):
            for d in PLANE_ORDER:
                send(h, d // NX, d % NX)

    def product_middle(r, h):
        for d in PLANE_ORDER:
            product_copy(r, h, 0, d, in_plane(d)).wait_recv()
        rows = slice(h * K // HALVES[r], (h + 1) * K // HALVES[r])
        total = product[r, here, rows]
        for d in range(1, PLANE):
            total = total + across[r, d, rows]
        return total

    def left(r):
        for i in range(CHUNKS):
            pair_copy(r, i).wait_send()
        for h in range(HALVES[r]):
            for d in PLANE_ORDER:
                product_copy(r, h, 0, d, in_plane(d)).wait_send()

        @pl.when(core == 1)
        def _():
            for d in PLANE_ORDER:
                gram_across(r, d).wait_send()
            for d in Z_ORDER:
                gram_deep(r, d, 1).wait_send()
            if r == 0:
                gram_pair().wait_send()
            else:
                for d in range(NZ):
                    gram_deep(r, d, 0).wait_send()

    def turn_over():
        def column(c, carry):
            for i in range(CHUNKS):
                strip = jnp.concatenate(
                    [jnp.transpose(x_ref[c, i * CHUNK + k * TILE : i * CHUNK + (k + 1) * TILE]) for k in range(CHUNK // TILE)],
                    axis=1,
                )
                xt_ref[i, c] = strip
            return carry

        lax.fori_loop(0, COL_BLOCKS, column, 0)

    build(0)
    for i in range(CHUNKS):
        chunk(
            0, i, lambda i: lax.dot_general(
                start[...], cells_of(i, range(COL_BLOCKS)), LANES, preferred_element_type=F32
            ),
        )
    join(0)
    gram_start(0)
    product_start(0)
    turn_over()
    gram_middle(0)
    def whole_copy(h, d):
        rows = pl.ds(h * K // HALVES[0], K // HALVES[0])
        return copy_of(deep_in.at[z, rows], deep_in.at[z, rows], DEEP + NZ * h + d, on_z(d, core))

    for h in range(HALVES[0]):
        deep_in[z, h * K // HALVES[0] : (h + 1) * K // HALVES[0]] = product_middle(0, h)
        for d in Z_ORDER:
            whole_copy(h, d).start()
    gram_end(0)
    for h in range(HALVES[0]):
        for d in Z_ORDER:
            whole_copy(h, d).wait_recv()
    total = deep_in[0]
    for zz in range(1, NZ):
        total = total + deep_in[zz]
    high, low = split(total)
    middle = jnp.dot(
        lower_ref[...], jnp.concatenate([high, low, high, low], axis=0), preferred_element_type=F32
    )
    mid[here] = middle.astype(BF16)

    def spread_copy(d):
        return copy_of(mid.at[here], mid.at[here], SPREAD + d, in_plane(d))

    for d in PLANE_ORDER:
        spread_copy(d).start()
    def scores_with(i, offsets):
        at = [NX * lax.rem(y + NY - d // NX, NY) + lax.rem(x + NX - d % NX, NX) for d in offsets]
        return lax.dot_general(
            jnp.concatenate([mid[n] for n in at], axis=1),
            jnp.concatenate([xt_ref[i, n] for n in at], axis=0), (((1,), (0,)), ((), ())),
            preferred_element_type=F32,
        )

    near, far = [0] + PLANE_ORDER[:3:-1], PLANE_ORDER[:4]
    for d in near[1:]:
        spread_copy(d).wait_recv()
    @pl.when(z >= 0)
    def _():
        for i in range(CHUNKS):
            partial[i] = scores_with(i, near)

    for d in far:
        spread_copy(d).wait_recv()
    for i in range(CHUNKS):
        chunk(1, i, lambda i: partial[i] + scores_with(i, far))
    join(1)
    gram_start(1)
    product_start(1)
    gram_middle(1)
    block = product_middle(1, 0)
    turned = jnp.transpose(jnp.concatenate([block, block], axis=0))
    lane_half = lax.broadcasted_iota(jnp.int32, (8, 2 * K), 1) < K
    for zz in range(NZ):
        pieces[zz] = jnp.where(lane_half, turned[16 * zz : 16 * zz + 8], turned[16 * zz + 8 : 16 * zz + 16])

    def piece_copy(d):
        peer = on_z(d, core)
        return copy_of(pieces.at[peer[2]], pieces_in.at[d], PER_ROUND + DEEP + d, peer)

    for d in Z_ORDER:
        piece_copy(d).start()
    gram_end(1)
    for d in Z_ORDER:
        piece_copy(d).wait_recv()
    piece = pieces[z]
    for d in range(1, NZ):
        piece = piece + pieces_in[d]
    piece_ref[...] = piece

    left(0)
    for h in range(HALVES[0]):
        for d in Z_ORDER:
            whole_copy(h, d).wait_send()
    for d in PLANE_ORDER:
        spread_copy(d).wait_send()
    left(1)
    for d in Z_ORDER:
        piece_copy(d).wait_send()


def local(tiles, tile_row, tile_col, tile_count, start_basis):
    vmem = pl.BlockSpec(memory_space=pltpu.VMEM)
    anywhere = pl.BlockSpec(memory_space=pltpu.HBM)
    parts = pl.pallas_call(
        kernel,
        out_shape=(
            pltpu.VMEM((K, 4 * K), BF16),
            pltpu.VMEM((2 * K, CELLS), BF16),
            pltpu.VMEM((8, TILE), F32),
        ),
        in_specs=[anywhere] * 5,
        out_specs=(vmem, vmem, vmem),
        scratch_shapes=[
            pltpu.VMEM((2, 1, SLOTS), jnp.int32),
            pltpu.VMEM((1, 1), jnp.int32),
            pltpu.VMEM((1, ROW_BLOCKS * COL_BLOCKS), jnp.int32),
            pltpu.SMEM((1, ROW_BLOCKS * COL_BLOCKS), jnp.int32),
            pltpu.VMEM((SLOTS + 1, TILE, TILE), BF16),
            pltpu.VMEM((COL_BLOCKS, CELLS, TILE), BF16),
            pltpu.VMEM((CHUNKS, COL_BLOCKS, TILE, CHUNK), BF16),
            pltpu.VMEM((K, GENES), BF16),
            pltpu.VMEM((2, CHUNKS, K, CHUNK), F32),
            pltpu.VMEM((2, CHUNKS, K, CHUNK), F32),
            pltpu.VMEM((2, PLANE, K, TILE), F32),
            pltpu.VMEM((2, PLANE, K, TILE), F32),
            pltpu.VMEM((NZ, K, TILE), F32),
            pltpu.VMEM((NZ, 8, TILE), F32),
            pltpu.VMEM((NZ, 8, TILE), F32),
            pltpu.VMEM((2, 24, 2 * K), F32),
            pltpu.VMEM((2, PLANE, 24, 2 * K), F32),
            pltpu.VMEM((2, NZ, 24, 2 * K), F32),
            pltpu.VMEM((24, 2 * K), F32),
            pltpu.VMEM((PLANE, K, TILE), BF16),
            pltpu.VMEM((CHUNKS, K, CHUNK), F32),
            pltpu.SemaphoreType.DMA((5 + LOADS,)),
            pltpu.SemaphoreType.DMA((MESSAGES,)),
            pltpu.SemaphoreType.DMA((MESSAGES,)),
        ],
        compiler_params=pltpu.CompilerParams(collective_id=0, has_side_effects=True),
    )(tile_row, tile_col, tile_count, tiles[0], start_basis)
    basis, loadings = pl.pallas_call(
        finish,
        out_shape=(
            jax.ShapeDtypeStruct((K, CELLS), BF16),
            jax.ShapeDtypeStruct((GENES // (PLANE * NZ), K), F32),
        ),
        in_specs=[vmem] * 3,
        out_specs=(vmem, vmem),
    )(*(pltpu.with_memory_space_constraint(part, pltpu.VMEM) for part in parts))
    return basis, loadings.T


def solution(mesh):
    finer = Mesh(
        mesh.devices.reshape(NY, NX, NZ, mesh.shape["gene"]), ("cell_0", "cell_1", "cell_2", "gene")
    )
    return jax.shard_map(
        local,
        mesh=finer,
        in_specs=(
            P("gene", CELL, None, None),
            P("gene", CELL),
            P("gene", CELL),
            P("gene", CELL),
            P(None, "gene"),
        ),
        out_specs=(P(None, CELL), P(None, GENE_CELL)),
        check_vma=False,
    )
```
